32 devices in a mesh: gene: 4 (over y, x), prot: 8 (over z, core).
Axes of the slice: x: 2, y: 2, z: 4, core: 2. Of those that a mesh axis runs over, the one named last changes fastest.
Arguments:
- density: float32 [256, 48, 16, 128], P('gene', 'prot'), may hold values from 0 to 2
- levels: float32 [8], replicated, may hold values from 0.1 to 0.9
- rate_index: int32 [256, 3], P('gene'), may hold values from 0 to 7
- on_rate: float32 [8], replicated, may hold values from 0.2 to 3
- off_rate: float32 [8], replicated, may hold values from 0.2 to 3
- gene_order: int32 [4], replicated, may hold values from 0 to 3, each once
Outputs:
- evolved: float32 [256, 48, 16, 128], P('gene', 'prot')
The draws below stay inside these ranges and needn't reach their ends.
Inputs may be any that keep to these rules, and one draw needn't show every extreme that they name: `gene_order`: a permutation of 0 to 3.
All inputs are finite; a program needn't handle non-finite values.
Results may differ from the reference program's by a relative error of at most 0.00002.
Values sent between devices are 32-bit elements; how exact they have to be, the bound alone decides.
A program may use at most 128 MiB of HBM per device.

```python
import math
import jax
import jax.numpy as jnp
from jax import lax

STATE_BITS = 8
LEVELS = 8
BLOCKS = 4
SUBSTEPS = 6
NY = 16
NZ = 128
STATES = 256
NX = 48


def touch_ends(values, stream_key, least, top_value):
    spot = [jax.random.randint(jax.random.fold_in(stream_key, axis), (), 0, length) for axis, length in enumerate(values.shape)]
    widest = values.shape.index(max(values.shape))
    neighbour = spot[:widest] + [(spot[widest] + 1) % values.shape[widest]] + spot[widest + 1:]
    return values.at[tuple(spot)].set(least).at[tuple(neighbour)].set(top_value)


def shard_levels(stream_key, shape, split, least, top_value):
    loudness, own = 1.0, jax.random.fold_in(stream_key, 6)
    for axis_at, parts in split:
        heights = jnp.exp(jax.random.uniform(jax.random.fold_in(own, axis_at), (parts,), jnp.float32, least / len(split), top_value / len(split)))
        loudness = loudness * jnp.repeat(heights, shape[axis_at] // parts).reshape([-1 if axis == axis_at else 1 for axis in range(len(shape))])
    return loudness


def setup_inputs(seed: int = 0) -> dict:
    splits = jax.random.split(jax.random.key(seed), 7)
    return {
        "density": jnp.clip(2.0 * jax.random.uniform(splits[0], (STATES, NX, NY, NZ), jnp.float32) ** shard_levels(splits[0], (STATES, NX, NY, NZ), ((0, 4), (1, 8)), -0.2, 0.2), 0.0, 2.0),
        "levels": jnp.clip(jax.random.uniform(splits[1], (LEVELS,), jnp.float32, 0.1, 0.9), 0.1, 0.9),
        "rate_index": touch_ends(jax.random.randint(splits[2], (STATES, 3), 0, LEVELS), jax.random.fold_in(splits[2], 1), 0, LEVELS - 1).astype(jnp.int32),
        "on_rate": jnp.clip(jnp.exp(jax.random.uniform(splits[3], (STATE_BITS,), jnp.float32, math.log(0.2), math.log(3.0))), 0.2, 3.0),
        "off_rate": jnp.clip(jnp.exp(jax.random.uniform(splits[4], (STATE_BITS,), jnp.float32, math.log(0.2), math.log(3.0))), 0.2, 3.0),
        "gene_order": jax.random.permutation(splits[5], BLOCKS).astype(jnp.int32),
    }


DIFF = 1.0
TIME_STEP = 0.15


def along(field, drift, axis):
    pads = [(0, 0)] * 4
    pads[axis] = (1, 1)
    padded = jnp.pad(field, pads)
    dpad = jnp.pad(drift, pads)
    size = field.shape[axis]
    upper = lax.slice_in_dim(padded, 2, size + 2, axis=axis)
    lower = lax.slice_in_dim(padded, 0, size, axis=axis)
    d_up = lax.slice_in_dim(dpad, 2, size + 2, axis=axis)
    d_low = lax.slice_in_dim(dpad, 0, size, axis=axis)
    return DIFF * (upper - 2.0 * field + lower) - 0.5 * (d_up * upper - d_low * lower)


def diffuse_group(pair):
    group_field, group_level = pair
    coord_x = (jnp.arange(NX, dtype=jnp.float32) + 0.5) / NX
    coord_y = (jnp.arange(NY, dtype=jnp.float32) + 0.5) / NY
    coord_z = (jnp.arange(NZ, dtype=jnp.float32) + 0.5) / NZ
    drift_x = (group_level[:, 0, None] - coord_x[None, :])[:, :, None, None]
    drift_y = (group_level[:, 1, None] - coord_y[None, :])[:, None, :, None]
    drift_z = (group_level[:, 2, None] - coord_z[None, :])[:, None, None, :]

    def one_step(step, field):
        change = along(field, drift_x, 1) + along(field, drift_y, 2) + along(field, drift_z, 3)
        return field + TIME_STEP * change

    return lax.fori_loop(0, SUBSTEPS, one_step, group_field)


def reference(density, levels, rate_index, on_rate, off_rate, gene_order):
    states = density.shape[0]
    groups = 16
    level_of = levels[rate_index]
    coord_x = (jnp.arange(NX, dtype=jnp.float32) + 0.5) / NX
    state_ids = jnp.arange(states, dtype=jnp.int32)
    hill = 0.1 + coord_x ** 2 / (0.09 + coord_x ** 2)
    grouped_level = level_of.reshape((groups, states // groups, 3))
    field = density
    for block in range(BLOCKS):
        grouped = field.reshape((groups, states // groups) + field.shape[1:])
        field = lax.map(diffuse_group, (grouped, grouped_level)).reshape(field.shape)
        bit = (STATE_BITS - 1 - gene_order[block]).astype(jnp.int32)
        mate_ids = jnp.bitwise_xor(state_ids, jnp.left_shift(jnp.int32(1), bit))
        mate = field[mate_ids]
        high = (jnp.bitwise_and(jnp.right_shift(state_ids, bit), 1) == 1)[:, None, None, None]
        act = (on_rate[bit] * hill)[None, :, None, None]
        rate = act + off_rate[bit]
        share = act / rate
        decay = jnp.exp(-rate)
        low_part = jnp.where(high, mate, field)
        high_part = jnp.where(high, field, mate)
        total = low_part + high_part
        new_high = share * total + (high_part - share * total) * decay
        field = jnp.where(high, new_high, total - new_high)
    return field
```

```python
from functools import partial

import jax
import jax.numpy as jnp
from jax import lax
from jax.experimental import pallas as pl
from jax.experimental.pallas import tpu as pltpu
from jax.sharding import PartitionSpec as P

STATE_BITS = 8
BLOCKS = 4
SUBSTEPS = 6
DIFF = 1.0
TIME_STEP = 0.15
KEEP = 1.0 - 6.0 * TIME_STEP * DIFF
TOP = 2**BLOCKS
PIECE = 16
MESH = pl.DeviceIdType.MESH


class Plan:
    def __init__(self, genes, prots, count, width, size_y, size_z):
        self.genes, self.prots = genes, prots
        self.units = count * genes // TOP
        self.mids = count // self.units
        self.slots = self.units // genes
        self.width, self.size_y, self.size_z = width, size_y, size_z
        self.total_x = width * prots
        self.halo = SUBSTEPS
        self.layers = width + 2 * self.halo
        assert self.slots * genes == self.units and self.mids * genes == TOP
        assert width >= self.halo


def body(
    pn, x_ref, rate_ref, levels_ref, on_ref, off_ref, order_ref, out_ref,
    near, post, work, rates, tab_x, tab_y, tab_z, tab_s,
    own_sem, halo_send, halo_recv, move_send, move_recv, out_send, out_recv, rate_send, rate_recv,
):
    g, p = lax.axis_index("gene"), lax.axis_index("prot")
    ny, nz = pn.size_y, pn.size_z
    genes, mids, slots, halo, width = pn.genes, pn.mids, pn.slots, pn.halo, pn.width
    has_left, has_right = p > 0, p < pn.prots - 1

    def rows(layer, n):
        return pl.ds(layer * ny, n * ny)

    def flip(a, d):
        out, bit = 0, 1
        while bit < genes:
            i, j = lax.rem(lax.div(a, bit), 2), lax.rem(lax.div(d, bit), 2)
            out = out + (i + j - 2 * i * j) * bit
            bit *= 2
        return out

    def order_of(j):
        return flip(g, genes - 1 - j)

    own, left_rows, right_rows = rows(halo, width), rows(0, halo), rows(halo + width, halo)

    barrier = pltpu.get_barrier_semaphore()

    def greet(d, carry):
        pl.semaphore_signal(barrier, inc=1, device_id=(flip(g, d), p), device_id_type=MESH)
        return carry

    lax.fori_loop(1, genes, greet, 0)

    @pl.when(has_left)
    def _():
        pl.semaphore_signal(barrier, inc=1, device_id=(g, p - 1), device_id_type=MESH)

    @pl.when(has_right)
    def _():
        pl.semaphore_signal(barrier, inc=1, device_id=(g, p + 1), device_id_type=MESH)

    pl.semaphore_wait(barrier, genes - 1 + jnp.where(has_left, 1, 0) + jnp.where(has_right, 1, 0))

    def edges(par, k, grp, from_input):
        def side(first, dst_rows, way, to):
            if from_input:
                src = x_ref.at[:, grp * slots + k, rows(first, halo)]
            else:
                src = near.at[par, k, grp, :, rows(halo + first, halo)]
            return pltpu.make_async_remote_copy(
                src_ref=src,
                dst_ref=near.at[par, k, grp, :, dst_rows],
                send_sem=halo_send.at[par, way, k, grp],
                recv_sem=halo_recv.at[par, way, k, grp],
                device_id=(g, to),
                device_id_type=MESH,
            )

        return side(width - halo, left_rows, 0, p + 1), side(0, right_rows, 1, p - 1)

    def send_edges(par, k, grp, from_input):
        to_right, to_left = edges(par, k, grp, from_input)
        pl.when(has_right)(to_right.start)
        pl.when(has_left)(to_left.start)

    def sent_edges(par, k, grp):
        to_right, to_left = edges(par, k, grp, False)
        pl.when(has_right)(to_right.wait_send)
        pl.when(has_left)(to_left.wait_send)

    def take_edges(par, k, grp):
        to_right, to_left = edges(par, k, grp, False)
        pl.when(has_left)(to_right.wait_recv)
        pl.when(has_right)(to_left.wait_recv)

    def own_copy(k, grp):
        return pltpu.make_async_copy(
            x_ref.at[:, grp * slots + k], near.at[0, k, grp, :, own], own_sem.at[k, grp]
        )

    def open_sub(i, carry):
        k, grp = lax.div(i, genes), order_of(lax.rem(i, genes))
        send_edges(0, k, grp, True)
        own_copy(k, grp).start()
        return carry

    lax.fori_loop(0, slots * genes, open_sub, 0)

    def rate_copy(to):
        return pltpu.make_async_remote_copy(
            src_ref=rate_ref,
            dst_ref=rates.at[g],
            send_sem=rate_send.at[to],
            recv_sem=rate_recv.at[g],
            device_id=(to, p),
            device_id_type=MESH,
        )

    def send_rates(d, carry):
        rate_copy(flip(g, d)).start()
        return carry

    lax.fori_loop(1, genes, send_rates, 0)

    cell = lax.broadcasted_iota(jnp.int32, (pn.layers * ny, nz), 0) // ny - halo + p * width
    inside = jnp.logical_and(cell >= 0, cell < pn.total_x)
    coord = (cell.astype(jnp.float32) + 0.5) / pn.total_x
    step_x = 1.0 / pn.total_x
    base, half = TIME_STEP * DIFF / KEEP, 0.5 * TIME_STEP / KEEP
    yi = lax.broadcasted_iota(jnp.int32, (ny, nz), 0)
    zi = lax.broadcasted_iota(jnp.int32, (8, nz), 1)
    y_at = (yi.astype(jnp.float32) + 0.5) / ny
    z_at = (zi.astype(jnp.float32) + 0.5) / nz

    def tables(l, carry):
        lev = levels_ref[l]
        tab_x[l, 0] = jnp.where(inside, base - half * (lev - (coord + step_x)), 0.0)
        tab_x[l, 1] = jnp.where(inside, base + half * (lev - (coord - step_x)), 0.0)
        tab_y[l, 0] = jnp.where(yi < ny - 1, base - half * (lev - (y_at + 1.0 / ny)), 0.0)
        tab_y[l, 1] = jnp.where(yi > 0, base + half * (lev - (y_at - 1.0 / ny)), 0.0)
        tab_z[l, 0] = jnp.where(zi < nz - 1, base - half * (lev - (z_at + 1.0 / nz)), 0.0)
        tab_z[l, 1] = jnp.where(zi > 0, base + half * (lev - (z_at - 1.0 / nz)), 0.0)
        return carry

    lax.fori_loop(0, levels_ref.shape[0], tables, 0)

    def blank(i, carry):
        par, k, grp = lax.div(i, slots * genes), lax.rem(lax.div(i, genes), slots), lax.rem(i, genes)
        zero = jnp.zeros((mids, halo * ny, nz), jnp.float32)

        @pl.when(jnp.logical_not(has_left))
        def _():
            near[par, k, grp, :, left_rows] = zero

        @pl.when(jnp.logical_not(has_right))
        def _():
            near[par, k, grp, :, right_rows] = zero

        return carry

    lax.fori_loop(0, 2 * slots * genes, blank, 0)

    scale = KEEP**SUBSTEPS
    own_cell = lax.broadcasted_iota(jnp.int32, (width, 8, nz), 0) + p * width
    own_x = (own_cell.astype(jnp.float32) + 0.5) / pn.total_x
    hill = 0.1 + own_x * own_x / (0.09 + own_x * own_x)
    for b in range(BLOCKS):
        bit = STATE_BITS - 1 - order_ref[b]
        act = on_ref[bit] * hill
        rate = act + off_ref[bit]
        share = act / rate
        gone = 1.0 - jnp.exp(-rate)
        up = share * gone
        down = (1.0 - share) * gone
        tab_s[b, 0, 0] = (1.0 - up) * scale
        tab_s[b, 0, 1] = down * scale
        tab_s[b, 1, 0] = (1.0 - down) * scale
        tab_s[b, 1, 1] = up * scale

    def own_rates(s, carry):
        for k in range(3):
            rates[g, k, s] = rate_ref[k, s]
        return carry

    lax.fori_loop(0, rate_ref.shape[1], own_rates, 0)

    def spread(src, start, n, c):
        at, size = start * ny, n * ny

        def read(off):
            return src[pl.ds(at + off, size)]

        here = read(0)
        out = here + c[0][pl.ds(at, size)] * read(ny) + c[1][pl.ds(at, size)] * read(-ny)
        by_y, by_z = (n, ny, nz), (size // 8, 8, nz)
        along_y = c[2][None] * read(1).reshape(by_y) + c[3][None] * read(-1).reshape(by_y)
        z_next = pltpu.roll(here, nz - 1, axis=1).reshape(by_z)
        z_last = pltpu.roll(here, 1, axis=1).reshape(by_z)
        along_z = c[4][None] * z_next + c[5][None] * z_last
        return out + along_y.reshape(size, nz) + along_z.reshape(size, nz)

    def diffuse(b, k, grp):
        first = b == 0
        who = jnp.where(first, g, grp)
        unit = jnp.where(first, grp * slots + k, g * slots + k)
        par, to = lax.rem(b, 2), jnp.minimum(b, 1)
        coef = []
        for m in range(mids):
            lev = [rates[who, d, m * pn.units + unit] for d in range(3)]
            coef.append(
                (
                    tab_x.at[lev[0], 0], tab_x.at[lev[0], 1], tab_y[lev[1], 0], tab_y[lev[1], 1],
                    tab_z[lev[2], 0], tab_z[lev[2], 1],
                )
            )
        for i in range(SUBSTEPS):
            extra = SUBSTEPS - 1 - i
            start, stop = halo - extra, halo + width + extra
            for at in range(start, stop, PIECE):
                n = min(PIECE, stop - at)
                for m in range(mids):
                    src = near.at[par, k, grp, m] if i == 0 else work.at[(i + 1) % 2, m]
                    new = spread(src, at, n, coef[m])
                    if i < SUBSTEPS - 1:
                        work[i % 2, m, rows(at, n)] = new
                    else:
                        post[to, k, grp, m, rows(at - halo, n)] = new

    def move(k, grp):
        return pltpu.make_async_remote_copy(
            src_ref=post.at[0, k, grp],
            dst_ref=post.at[1, k, g],
            send_sem=move_send.at[k, grp],
            recv_sem=move_recv.at[k, g],
            device_id=(grp, p),
            device_id_type=MESH,
        )

    def local_wait(k, grp, sem):
        pltpu.make_async_copy(post.at[0, k, grp], post.at[1, k, grp], sem).wait()

    def sub(b, k, j):
        grp = order_of(j)
        take_edges(lax.rem(b, 2), k, grp)
        first, last = b == 0, j == genes - 1

        @pl.when(first)
        def _():
            own_copy(k, grp).wait()

        diffuse(b, k, grp)

        @pl.when(jnp.logical_and(first, jnp.logical_not(last)))
        def _():
            move(k, grp).start()

        @pl.when(jnp.logical_and(first, last))
        def _():
            post[1, k, g] = post[0, k, g]

    def out_copy(k, grp):
        return pltpu.make_async_remote_copy(
            src_ref=near.at[BLOCKS % 2, k, grp, :, own],
            dst_ref=out_ref.at[:, g * slots + k],
            send_sem=out_send.at[k, grp],
            recv_sem=out_recv.at[k, g],
            device_id=(grp, p),
            device_id_type=MESH,
        )

    def keep_copy(k):
        return pltpu.make_async_copy(
            near.at[BLOCKS % 2, k, g, :, own], out_ref.at[:, g * slots + k], out_recv.at[k, g]
        )

    def switch(i, carry):
        b, k = lax.div(i, slots), lax.rem(i, slots)
        par = lax.rem(b + 1, 2)

        @pl.when(b == 0)
        def _():
            def arrived(d, c):
                grp = flip(g, d)
                local_wait(k, grp, move_recv.at[k, grp])
                return c

            lax.fori_loop(1, genes, arrived, 0)

        @pl.when(b > 0)
        def _():
            lax.fori_loop(0, genes, lambda grp, c: (sent_edges(par, k, grp), c)[1], 0)

        order = order_ref[b]
        picks = [order == q for q in range(BLOCKS)]
        masks = [TOP >> (q + 1) for q in range(BLOCKS)]

        def of_mask(values):
            out = values[-1]
            for q in range(BLOCKS - 1):
                out = lax.select(picks[q], values[q], out)
            return out

        high = [of_mask([jnp.int32(1 if t & mask else 0) for mask in masks]) for t in range(TOP)]

        def strip(r, c):
            layer = lax.div(r * 8, ny)
            at = pl.ds(pl.multiple_of(r * 8, 8), 8)
            to = pl.ds(pl.multiple_of(halo * ny + r * 8, 8), 8)
            held = [post[1, k, t // mids, t % mids, at] for t in range(TOP)]
            for t in range(TOP):
                mate = of_mask([held[t ^ mask] for mask in masks])
                near[par, k, t // mids, t % mids, to] = (
                    tab_s[b, high[t], 0, layer] * held[t] + tab_s[b, high[t], 1, layer] * mate
                )
            return c

        lax.fori_loop(0, width * ny // 8, strip, 0)

        @pl.when(b < BLOCKS - 1)
        def _():
            lax.fori_loop(0, genes, lambda j, c: (send_edges(par, k, order_of(j), False), c)[1], 0)

        @pl.when(b == BLOCKS - 1)
        def _():
            lax.fori_loop(0, genes - 1, lambda j, c: (out_copy(k, order_of(j)).start(), c)[1], 0)
            keep_copy(k).start()

        return carry

    def step(i, carry):
        b, k = lax.div(i, slots), lax.rem(i, slots)
        lax.fori_loop(0, genes, lambda j, c: (sub(b, k, j), c)[1], 0)

        @pl.when(i == slots - 1)
        def _():
            def arrived(d, c):
                grp = flip(g, d)
                pltpu.make_async_copy(rates.at[grp], rates.at[grp], rate_recv.at[grp]).wait()
                return c

            lax.fori_loop(1, genes, arrived, 0)

        first, last = b == 0, k == slots - 1
        begin = jnp.where(first, jnp.maximum(k - 1, 0), i)
        end = jnp.where(first, jnp.where(last, k + 1, k), i + 1)
        lax.fori_loop(begin, end, switch, 0)
        return carry

    lax.fori_loop(0, BLOCKS * slots, step, 0)

    def finish(i, carry):
        k, grp = lax.div(i, genes), lax.rem(i, genes)
        sent_edges(1 - BLOCKS % 2, k, grp)

        @pl.when(grp != g)
        def _():
            local_wait(k, grp, move_send.at[k, grp])
            out_copy(k, grp).wait_send()

        pltpu.make_async_copy(
            near.at[BLOCKS % 2, k, grp, :, own], out_ref.at[:, grp * slots + k], out_recv.at[k, grp]
        ).wait()
        return carry

    lax.fori_loop(0, slots * genes, finish, 0)
    lax.fori_loop(1, genes, lambda d, c: (rate_copy(flip(g, d)).wait_send(), c)[1], 0)


def local(density, levels, rate_index, on_rate, off_rate, gene_order):
    count, width_x, size_y, size_z = density.shape
    pn = Plan(lax.axis_size("gene"), lax.axis_size("prot"), count, width_x, size_y, size_z)
    shape = (pn.mids, pn.units, width_x * size_y, size_z)
    smem = pl.BlockSpec(memory_space=pltpu.SMEM)
    hbm = pl.BlockSpec(memory_space=pl.ANY)
    f32 = jnp.float32
    tall = (pn.layers * size_y, size_z)
    per_sub = (pn.slots, pn.genes)
    dma = pltpu.SemaphoreType.DMA
    out = pl.pallas_call(
        partial(body, pn),
        out_shape=jax.ShapeDtypeStruct(shape, f32),
        in_specs=[hbm] + [smem] * 5,
        out_specs=hbm,
        scratch_shapes=[
            pltpu.VMEM((2,) + per_sub + (pn.mids,) + tall, f32),
            pltpu.VMEM((2,) + per_sub + (pn.mids, width_x * size_y, size_z), f32),
            pltpu.VMEM((2, pn.mids) + tall, f32),
            pltpu.SMEM((pn.genes, 3, count), jnp.int32),
            pltpu.VMEM(levels.shape + (2,) + tall, f32),
            pltpu.VMEM(levels.shape + (2, size_y, size_z), f32),
            pltpu.VMEM(levels.shape + (2, 8, size_z), f32),
            pltpu.VMEM((BLOCKS, 2, 2, width_x, 8, size_z), f32),
            dma(per_sub),
            dma((2, 2) + per_sub),
            dma((2, 2) + per_sub),
            dma(per_sub),
            dma(per_sub),
            dma(per_sub),
            dma(per_sub),
            dma((pn.genes,)),
            dma((pn.genes,)),
        ],
        compiler_params=pltpu.CompilerParams(
            collective_id=0, has_side_effects=True, vmem_limit_bytes=60 * 1024 * 1024
        ),
        name="exchange_evolve",
    )(density.reshape(shape), rate_index.T, levels, on_rate, off_rate, gene_order)
    return out.reshape(density.shape)


def solution(mesh):
    in_specs = (P("gene", "prot", None, None), P(), P("gene", None), P(), P(), P())
    out_specs = P("gene", "prot", None, None)
    return jax.shard_map(local, mesh=mesh, in_specs=in_specs, out_specs=out_specs, check_vma=False)
```

```python
from functools import partial

import jax
import jax.numpy as jnp
from jax import lax
from jax.experimental import pallas as pl
from jax.experimental.pallas import tpu as pltpu
from jax.sharding import PartitionSpec as P

STATE_BITS = 8
BLOCKS = 4
SUBSTEPS = 6
DIFF = 1.0
TIME_STEP = 0.15
KEEP = 1.0 - 6.0 * TIME_STEP * DIFF
TOP = 2**BLOCKS
BATCH = 2
PIECE = 16
ORDER = (12, 8, 4, 13, 14, 9, 5, 15, 10, 6, 11, 7, 0, 1, 2, 3)
MASKS = tuple(TOP >> (q + 1) for q in range(BLOCKS))
MESH = pl.DeviceIdType.MESH


def final_after():
    batch_of = {r: s // BATCH for s, r in enumerate(ORDER)}
    last = {r: max(batch_of[a] for a in [r] + [r ^ mask for mask in MASKS]) for r in range(TOP)}
    return [[r for r in ORDER if last[r] == i] for i in range(TOP // BATCH)]


class Plan:
    def __init__(self, genes, prots, count, width, size_y, size_z):
        self.genes, self.prots = genes, prots
        self.units = count * genes // TOP
        self.mids = count // self.units
        self.slots = self.units // genes
        self.width, self.size_y, self.size_z = width, size_y, size_z
        self.total_x = width * prots
        self.halo = SUBSTEPS
        self.layers = width + 2 * self.halo
        assert self.slots * genes == self.units and self.mids * genes == TOP
        assert width >= self.halo


def body(
    pn, x_ref, rate_ref, levels_ref, on_ref, off_ref, order_ref, out_ref,
    near, post, work, tab_x, tab_y, tab_z, tab_s, rates, levels, on, off, gene_order, lev_tab,
    small_sem, own_sem, halo_send, halo_recv, move_send, move_recv, out_send, out_recv, rate_send, rate_recv,
):
    g, p = lax.axis_index("gene"), lax.axis_index("prot")
    ny, nz = pn.size_y, pn.size_z
    genes, mids, slots, halo, width = pn.genes, pn.mids, pn.slots, pn.halo, pn.width
    has_left, has_right = p > 0, p < pn.prots - 1
    batches = TOP // BATCH
    away = (genes - 1) * mids

    def rows(layer, n):
        return pl.ds(layer * ny, n * ny)

    def flip(a, d):
        out, bit = 0, 1
        while bit < genes:
            i, j = lax.rem(lax.div(a, bit), 2), lax.rem(lax.div(d, bit), 2)
            out = out + (i + j - 2 * i * j) * bit
            bit *= 2
        return out

    peers = [g] + [flip(g, d) for d in range(1, genes)]
    own, left_rows, right_rows = rows(halo, width), rows(0, halo), rows(halo + width, halo)

    small = [
        pltpu.make_async_copy(src, dst, small_sem.at[i])
        for i, (src, dst) in enumerate(
            [
                (rate_ref, rates.at[g]), (levels_ref, levels), (on_ref, on), (off_ref, off),
                (order_ref, gene_order),
            ]
        )
    ]
    for copy in small:
        copy.start()

    barrier = pltpu.get_barrier_semaphore()
    for d in range(1, genes):
        pl.semaphore_signal(barrier, inc=1, device_id=(peers[d], p), device_id_type=MESH)

    @pl.when(has_left)
    def _():
        pl.semaphore_signal(barrier, inc=1, device_id=(g, p - 1), device_id_type=MESH)

    @pl.when(has_right)
    def _():
        pl.semaphore_signal(barrier, inc=1, device_id=(g, p + 1), device_id_type=MESH)

    pl.semaphore_wait(barrier, genes - 1 + jnp.where(has_left, 1, 0) + jnp.where(has_right, 1, 0))

    def edge(src, par, way, k, batch, where):
        return pltpu.make_async_remote_copy(
            src_ref=src,
            dst_ref=near.at[par, k, where, right_rows if way else left_rows],
            send_sem=halo_send.at[par, way, k],
            recv_sem=halo_recv.at[par, way, k, batch],
            device_id=(g, p - 1 if way else p + 1),
            device_id_type=MESH,
        )

    first_layer = (width - halo, 0)
    can_send, can_take = (has_right, has_left), (has_left, has_right)

    def send_edges(par, k, batch):
        where = pl.ds(batch * BATCH, BATCH)
        for way in range(2):
            src = near.at[par, k, where, rows(halo + first_layer[way], halo)]
            pl.when(can_send[way])(edge(src, par, way, k, batch, where).start)

    def sent_edges(par, k):
        for way in range(2):
            src = near.at[par, k, :, left_rows]
            pl.when(can_send[way])(pltpu.make_async_copy(src, src, halo_send.at[par, way, k]).wait)

    def take_edges(par, k, batch):
        for way in range(2):
            dst = near.at[par, k, pl.ds(batch * BATCH, BATCH), right_rows if way else left_rows]
            pl.when(can_take[way])(pltpu.make_async_copy(dst, dst, halo_recv.at[par, way, k, batch]).wait)

    def own_copy(k, s):
        unit = peers[ORDER[s] // mids] * slots + k
        return pltpu.make_async_copy(
            x_ref.at[ORDER[s] % mids, unit], near.at[0, k, s, own], own_sem.at[k, s // BATCH]
        )

    def open_slot(k, carry):
        for way in range(2):

            @pl.when(can_send[way])
            def _(way=way):
                for s, r in enumerate(ORDER):
                    unit = peers[r // mids] * slots + k
                    src = x_ref.at[r % mids, unit, rows(first_layer[way], halo)]
                    edge(src, 0, way, k, s // BATCH, s).start()

        for s in range(TOP):
            own_copy(k, s).start()
        return carry

    lax.fori_loop(0, slots, open_slot, 0)
    for copy in small:
        copy.wait()

    def rate_copy(d):
        return pltpu.make_async_remote_copy(
            src_ref=rates.at[g],
            dst_ref=rates.at[g],
            send_sem=rate_send.at[d],
            recv_sem=rate_recv.at[d],
            device_id=(peers[d], p),
            device_id_type=MESH,
        )

    for d in range(1, genes):
        rate_copy(d).start()

    def look_up(late, k):
        for s, r in enumerate(ORDER):
            who, unit = (peers[r // mids], g * slots + k) if late else (g, peers[r // mids] * slots + k)
            for d in range(3):
                lev_tab[((late * slots + k) * TOP + s) * 3 + d] = rates[who, d, r % mids * pn.units + unit]

    lax.fori_loop(0, slots, lambda k, c: (look_up(0, k), c)[1], 0)

    cell = lax.broadcasted_iota(jnp.int32, (pn.layers * ny, nz), 0) // ny - halo + p * width
    inside = jnp.logical_and(cell >= 0, cell < pn.total_x)
    coord = (cell.astype(jnp.float32) + 0.5) / pn.total_x
    step_x = 1.0 / pn.total_x
    base, half = TIME_STEP * DIFF / KEEP, 0.5 * TIME_STEP / KEEP
    yi = lax.broadcasted_iota(jnp.int32, (ny, nz), 0)
    zi = lax.broadcasted_iota(jnp.int32, (8, nz), 1)
    y_at = (yi.astype(jnp.float32) + 0.5) / ny
    z_at = (zi.astype(jnp.float32) + 0.5) / nz

    def tables(l, carry):
        lev = levels[l]
        tab_x[l, 0] = jnp.where(inside, base - half * (lev - (coord + step_x)), 0.0)
        tab_x[l, 1] = jnp.where(inside, base + half * (lev - (coord - step_x)), 0.0)
        tab_y[l, 0] = jnp.where(yi < ny - 1, base - half * (lev - (y_at + 1.0 / ny)), 0.0)
        tab_y[l, 1] = jnp.where(yi > 0, base + half * (lev - (y_at - 1.0 / ny)), 0.0)
        tab_z[l, 0] = jnp.where(zi < nz - 1, base - half * (lev - (z_at + 1.0 / nz)), 0.0)
        tab_z[l, 1] = jnp.where(zi > 0, base + half * (lev - (z_at - 1.0 / nz)), 0.0)
        return carry

    lax.fori_loop(0, levels_ref.shape[0], tables, 0)

    def blank(i, carry):
        par, k, s = lax.div(i, slots * TOP), lax.rem(lax.div(i, TOP), slots), lax.rem(i, TOP)
        zero = jnp.zeros((halo * ny, nz), jnp.float32)

        @pl.when(jnp.logical_not(has_left))
        def _():
            near[par, k, s, left_rows] = zero

        @pl.when(jnp.logical_not(has_right))
        def _():
            near[par, k, s, right_rows] = zero

        return carry

    lax.fori_loop(0, 2 * slots * TOP, blank, 0)

    scale = KEEP**SUBSTEPS
    own_cell = lax.broadcasted_iota(jnp.int32, (width, 8, nz), 0) + p * width
    own_x = (own_cell.astype(jnp.float32) + 0.5) / pn.total_x
    hill = 0.1 + own_x * own_x / (0.09 + own_x * own_x)
    for b in range(BLOCKS):
        bit = STATE_BITS - 1 - gene_order[b]
        act = on[bit] * hill
        rate = act + off[bit]
        share = act / rate
        gone = 1.0 - jnp.exp(-rate)
        up = share * gone
        down = (1.0 - share) * gone
        tab_s[b, 0, 0] = (1.0 - up) * scale
        tab_s[b, 0, 1] = down * scale
        tab_s[b, 1, 0] = (1.0 - down) * scale
        tab_s[b, 1, 1] = up * scale

    def spread(src, start, n, c):
        at, size = start * ny, n * ny

        def read(off):
            return src[pl.ds(at + off, size)]

        here = read(0)
        out = here + c[0][pl.ds(at, size)] * read(ny) + c[1][pl.ds(at, size)] * read(-ny)
        by_y, by_z = (n, ny, nz), (size // 8, 8, nz)
        along_y = c[2][None] * read(1).reshape(by_y) + c[3][None] * read(-1).reshape(by_y)
        z_next = pltpu.roll(here, nz - 1, axis=1).reshape(by_z)
        z_last = pltpu.roll(here, 1, axis=1).reshape(by_z)
        along_z = c[4][None] * z_next + c[5][None] * z_last
        return out + along_y.reshape(size, nz) + along_z.reshape(size, nz)

    def diffuse(b, k, batch):
        par, to = lax.rem(b, 2), jnp.minimum(b, 1)
        coef = []
        for m in range(BATCH):
            at = ((to * slots + k) * TOP + batch * BATCH + m) * 3
            lev = [lev_tab[at + d] for d in range(3)]
            coef.append(
                (
                    tab_x.at[lev[0], 0], tab_x.at[lev[0], 1], tab_y[lev[1], 0], tab_y[lev[1], 1],
                    tab_z[lev[2], 0], tab_z[lev[2], 1],
                )
            )
        for i in range(SUBSTEPS):
            extra = SUBSTEPS - 1 - i
            start, stop = halo - extra, halo + width + extra
            for at in range(start, stop, PIECE):
                n = min(PIECE, stop - at)
                for m in range(BATCH):
                    s = batch * BATCH + m
                    src = near.at[par, k, s] if i == 0 else work.at[(i + 1) % 2, m]
                    new = spread(src, at, n, coef[m])
                    if i < SUBSTEPS - 1:
                        work[i % 2, m, rows(at, n)] = new
                    else:
                        post[to, k, s, rows(at - halo, n)] = new

    def move(k, s):
        return pltpu.make_async_remote_copy(
            src_ref=post.at[0, k, s],
            dst_ref=post.at[1, k, s],
            send_sem=move_send,
            recv_sem=move_recv.at[k],
            device_id=(peers[ORDER[s] // mids], p),
            device_id_type=MESH,
        )

    def picked(b):
        order = gene_order[b]
        picks = [order == q for q in range(BLOCKS)]

        def of_mask(values):
            out = values[-1]
            for q in range(BLOCKS - 1):
                out = lax.select(picks[q], values[q], out)
            return out

        return of_mask

    def is_high(of_mask, r):
        values = []
        for mask in MASKS:
            bit = jnp.int32(1 if r & mask else 0)
            if mask >= mids:
                mine = lax.rem(lax.div(g, mask // mids), 2)
                bit = 1 - mine if r & mask else mine
            values.append(bit)
        return of_mask(values)

    def mix(b, k, states, store):
        of_mask = picked(b)
        high = {r: is_high(of_mask, r) for r in states}
        wanted = [r for r in range(TOP) if r in states or any(r ^ mask in states for mask in MASKS)]

        def strip(i, c):
            layer = lax.div(i * 8, ny)
            at = pl.multiple_of(i * 8, 8)
            held = {r: post[1, k, ORDER.index(r), pl.ds(at, 8)] for r in wanted}
            for r in states:
                mate = of_mask([held[r ^ mask] for mask in MASKS])
                store(r, at, tab_s[b, high[r], 0, layer] * held[r] + tab_s[b, high[r], 1, layer] * mate)
            return c

        lax.fori_loop(0, width * ny // 8, strip, 0)

    def place(par, k):
        def store(r, at, value):
            near[par, k, ORDER.index(r), pl.ds(pl.multiple_of(halo * ny + at, 8), 8)] = value

        return store

    def switch(i, carry):
        b, k = lax.div(i, slots), lax.rem(i, slots)
        par = lax.rem(b + 1, 2)

        @pl.when(b == 0)
        def _():
            dst = post.at[1, k, pl.ds(0, away)]
            pltpu.make_async_copy(dst, dst, move_recv.at[k]).wait()

        pl.when(b > 0)(lambda: sent_edges(par, k))
        mix(b, k, list(range(TOP)), place(par, k))
        lax.fori_loop(0, batches, lambda batch, c: (send_edges(par, k, batch), c)[1], 0)
        return carry

    end_par = BLOCKS % 2

    def out_copy(k, r):
        return pltpu.make_async_remote_copy(
            src_ref=near.at[end_par, k, ORDER.index(r), own],
            dst_ref=out_ref.at[r % mids, g * slots + k],
            send_sem=out_send,
            recv_sem=out_recv,
            device_id=(peers[r // mids], p),
            device_id_type=MESH,
        )

    def finish_states(k, states):
        sent = [r for r in states if r >= mids]
        kept = [r for r in states if r < mids]
        if sent:
            mix(BLOCKS - 1, k, sent, place(end_par, k))
            for r in sent:
                out_copy(k, r).start()

        def keep(r, at, value):
            out_ref[r, g * slots + k, pl.ds(at, 8)] = value

        if kept:
            mix(BLOCKS - 1, k, kept, keep)

    finals = final_after()
    opening = min(i for i in range(batches) if finals[i])

    def sub(b, k, batch):
        take_edges(lax.rem(b, 2), k, batch)
        first = b == 0

        @pl.when(first)
        def _():
            dst = near.at[0, k, pl.ds(batch * BATCH, BATCH), own]
            pltpu.make_async_copy(dst, dst, own_sem.at[k, batch]).wait()

        diffuse(b, k, batch)
        for i in range(batches):

            @pl.when(jnp.logical_and(first, batch == i))
            def _(i=i):
                for s in range(i * BATCH, (i + 1) * BATCH):
                    if ORDER[s] >= mids:
                        move(k, s).start()
                    else:
                        post[1, k, s] = post[0, k, s]

            if finals[i]:

                @pl.when(jnp.logical_and(b == BLOCKS - 1, batch == i))
                def _(i=i):
                    if i == opening:
                        sent_edges(end_par, k)
                    finish_states(k, finals[i])

    def step(i, carry):
        b, k = lax.div(i, slots), lax.rem(i, slots)
        lax.fori_loop(0, batches, lambda batch, c: (sub(b, k, batch), c)[1], 0)

        @pl.when(i == slots - 1)
        def _():
            for d in range(1, genes):
                dst = rates.at[peers[d]]
                pltpu.make_async_copy(dst, dst, rate_recv.at[d]).wait()
            lax.fori_loop(0, slots, lambda q, c: (look_up(1, q), c)[1], 0)

        first, last, end = b == 0, k == slots - 1, b == BLOCKS - 1
        start = jnp.where(first, jnp.maximum(k - 1, 0), i)
        stop = jnp.where(first, jnp.where(last, k + 1, k), jnp.where(end, i, i + 1))
        lax.fori_loop(start, stop, switch, 0)
        return carry

    lax.fori_loop(0, BLOCKS * slots, step, 0)

    lax.fori_loop(0, slots, lambda k, c: (sent_edges(1 - end_par, k), c)[1], 0)
    src = post.at[0, :, pl.ds(0, away)]
    pltpu.make_async_copy(src, src, move_send).wait()
    for d in range(1, genes):
        rate_copy(d).wait_send()
    src = near.at[end_par, :, pl.ds(0, away), own]
    pltpu.make_async_copy(src, src, out_send).wait()
    dst = out_ref.at[:, pl.ds(0, (genes - 1) * slots)]
    pltpu.make_async_copy(dst, dst, out_recv).wait()


def local(density, levels, rate_index, on_rate, off_rate, gene_order):
    count, width_x, size_y, size_z = density.shape
    pn = Plan(lax.axis_size("gene"), lax.axis_size("prot"), count, width_x, size_y, size_z)
    shape = (pn.mids, pn.units, width_x * size_y, size_z)
    inputs = (density.reshape(shape), rate_index.T, levels, on_rate, off_rate, gene_order)
    f32, i32 = jnp.float32, jnp.int32
    tall = (pn.layers * size_y, size_z)
    dma = pltpu.SemaphoreType.DMA
    out = pl.pallas_call(
        partial(body, pn),
        out_shape=pltpu.VMEM(shape, f32),
        in_specs=[pl.BlockSpec(memory_space=pltpu.HBM)] * len(inputs),
        out_specs=pl.BlockSpec(memory_space=pltpu.VMEM),
        scratch_shapes=[
            pltpu.VMEM((2, pn.slots, TOP) + tall, f32),
            pltpu.VMEM((2, pn.slots, TOP, width_x * size_y, size_z), f32),
            pltpu.VMEM((2, BATCH) + tall, f32),
            pltpu.VMEM(levels.shape + (2,) + tall, f32),
            pltpu.VMEM(levels.shape + (2, size_y, size_z), f32),
            pltpu.VMEM(levels.shape + (2, 8, size_z), f32),
            pltpu.VMEM((BLOCKS, 2, 2, width_x, 8, size_z), f32),
            pltpu.SMEM((pn.genes, 3, count), i32),
            pltpu.SMEM(levels.shape, f32),
            pltpu.SMEM(on_rate.shape, f32),
            pltpu.SMEM(off_rate.shape, f32),
            pltpu.SMEM(gene_order.shape, i32),
            pltpu.SMEM((2 * pn.slots * TOP * 3,), i32),
            dma((len(inputs) - 1,)),
            dma((pn.slots, TOP // BATCH)),
            dma((2, 2, pn.slots)),
            dma((2, 2, pn.slots, TOP // BATCH)),
            dma(()),
            dma((pn.slots,)),
            dma(()),
            dma(()),
            dma((pn.genes,)),
            dma((pn.genes,)),
        ],
        compiler_params=pltpu.CompilerParams(
            collective_id=0, has_side_effects=True, vmem_limit_bytes=56 * 1024 * 1024
        ),
        name="exchange_evolve",
    )(*[pltpu.with_memory_space_constraint(a, pltpu.HBM) for a in inputs])
    return out.reshape(density.shape)


def solution(mesh):
    in_specs = (P("gene", "prot", None, None), P(), P("gene", None), P(), P(), P())
    out_specs = P("gene", "prot", None, None)
    return jax.shard_map(local, mesh=mesh, in_specs=in_specs, out_specs=out_specs, check_vma=False)
```

```python
from functools import partial

import jax
import jax.numpy as jnp
from jax import lax
from jax.experimental import pallas as pl
from jax.experimental.pallas import tpu as pltpu
from jax.sharding import PartitionSpec as P

STATE_BITS = 8
BLOCKS = 4
SUBSTEPS = 6
DIFF = 1.0
TIME_STEP = 0.15
KEEP = 1.0 - 6.0 * TIME_STEP * DIFF
TOP = 2**BLOCKS
BATCH = 2
PIECE = 2
ORDER = (12, 8, 4, 13, 14, 9, 5, 15, 10, 6, 11, 7, 0, 1, 2, 3)
MASKS = tuple(TOP >> (q + 1) for q in range(BLOCKS))
MESH = pl.DeviceIdType.MESH


def final_after():
    batch_of = {r: s // BATCH for s, r in enumerate(ORDER)}
    last = {r: max(batch_of[a] for a in [r] + [r ^ mask for mask in MASKS]) for r in range(TOP)}
    return [[r for r in ORDER if last[r] == i] for i in range(TOP // BATCH)]


class Plan:
    def __init__(self, genes, prots, count, width, size_y, size_z):
        self.genes, self.prots = genes, prots
        self.units = count * genes // TOP
        self.mids = count // self.units
        self.slots = self.units // genes
        self.width, self.size_y, self.size_z = width, size_y, size_z
        self.total_x = width * prots
        self.halo = SUBSTEPS
        self.layers = width + 2 * self.halo
        assert self.slots * genes == self.units and self.mids * genes == TOP
        assert width >= self.halo


def body(
    pn, x_ref, rate_ref, levels_ref, on_ref, off_ref, order_ref, out_ref,
    near, post, work, tab_x, tab_y, tab_z, tab_s, rates, levels, on, off, gene_order, lev_tab,
    small_sem, own_sem, halo_send, halo_recv, last_recv, move_send, move_recv, out_send, out_recv, rate_send, rate_recv,
):
    g, p = lax.axis_index("gene"), lax.axis_index("prot")
    ny, nz = pn.size_y, pn.size_z
    genes, mids, slots, halo, width = pn.genes, pn.mids, pn.slots, pn.halo, pn.width
    has_left, has_right = p > 0, p < pn.prots - 1
    has_both = jnp.logical_and(has_left, has_right)
    has_one = jnp.logical_and(jnp.logical_or(has_left, has_right), jnp.logical_not(has_both))
    near_genes = [1 << i for i in range(genes.bit_length() - 1)]
    batches = TOP // BATCH
    away = (genes - 1) * mids

    def rows(layer, n):
        return pl.ds(layer * ny, n * ny)

    def flip(a, d):
        out, bit = 0, 1
        while bit < genes:
            i, j = lax.rem(lax.div(a, bit), 2), lax.rem(lax.div(d, bit), 2)
            out = out + (i + j - 2 * i * j) * bit
            bit *= 2
        return out

    peers = [g] + [flip(g, d) for d in range(1, genes)]
    own, left_rows, right_rows = rows(halo, width), rows(0, halo), rows(halo + width, halo)

    small = [
        pltpu.make_async_copy(src, dst, small_sem.at[i])
        for i, (src, dst) in enumerate(
            [
                (rate_ref, rates.at[0]), (levels_ref, levels), (on_ref, on), (off_ref, off),
                (order_ref, gene_order),
            ]
        )
    ]
    for copy in small:
        copy.start()

    barrier = pltpu.get_barrier_semaphore()
    for d in near_genes:
        pl.semaphore_signal(barrier, inc=1, device_id=(peers[d], p), device_id_type=MESH)

    @pl.when(has_left)
    def _():
        pl.semaphore_signal(barrier, inc=1, device_id=(g, p - 1), device_id_type=MESH)

    @pl.when(has_right)
    def _():
        pl.semaphore_signal(barrier, inc=1, device_id=(g, p + 1), device_id_type=MESH)

    pl.semaphore_wait(barrier, len(near_genes) + jnp.where(has_left, 1, 0) + jnp.where(has_right, 1, 0))

    def edge(src, par, way, k, where, recv_sem):
        return pltpu.make_async_remote_copy(
            src_ref=src,
            dst_ref=near.at[par, k, where, right_rows if way else left_rows],
            send_sem=halo_send.at[par],
            recv_sem=recv_sem,
            device_id=(g, p - 1 if way else p + 1),
            device_id_type=MESH,
        )

    first_layer = (width - halo, 0)
    can_send = (has_right, has_left)

    def send_edges(par, k, where, recv_sem):
        for way in range(2):
            src = near.at[par, k, where, rows(halo + first_layer[way], halo)]
            pl.when(can_send[way])(edge(src, par, way, k, where, recv_sem).start)

    def both_ways(ref_of, sem):
        one, two = ref_of(rows(0, halo)), ref_of(rows(0, 2 * halo))
        pl.when(has_one)(pltpu.make_async_copy(one, one, sem).wait)
        pl.when(has_both)(pltpu.make_async_copy(two, two, sem).wait)

    def sent_edges(par):
        both_ways(lambda at: near.at[par, :, :, at], halo_send.at[par])

    def own_copy(k, s):
        unit = peers[ORDER[s] // mids] * slots + k
        return pltpu.make_async_copy(
            x_ref.at[ORDER[s] % mids, unit], near.at[0, k, s, own], own_sem
        )

    def open_slot(k, carry):
        for way in range(2):

            @pl.when(can_send[way])
            def _(way=way):
                for s, r in enumerate(ORDER):
                    unit = peers[r // mids] * slots + k
                    src = x_ref.at[r % mids, unit, rows(first_layer[way], halo)]
                    edge(src, 0, way, k, s, halo_recv.at[0, k]).start()

        for s in range(TOP):
            own_copy(k, s).start()
        return carry

    lax.fori_loop(0, slots, open_slot, 0)
    for copy in small:
        copy.wait()

    def rate_copy(i):
        return pltpu.make_async_remote_copy(
            src_ref=rates.at[pl.ds(0, near_genes[i])],
            dst_ref=rates.at[pl.ds(near_genes[i], near_genes[i])],
            send_sem=rate_send,
            recv_sem=rate_recv.at[i],
            device_id=(peers[near_genes[i]], p),
            device_id_type=MESH,
        )

    def look_up(late, k):
        for s, r in enumerate(ORDER):
            row = r // mids if late else 0
            unit = (g if late else peers[r // mids]) * slots + k
            for d in range(3):
                lev_tab[((late * slots + k) * TOP + s) * 3 + d] = rates[row, d, r % mids * pn.units + unit]

    rate_copy(0).start()
    lax.fori_loop(0, slots, lambda k, c: (look_up(0, k), c)[1], 0)

    cell = lax.broadcasted_iota(jnp.int32, (pn.layers * ny, nz), 0) // ny - halo + p * width
    inside = jnp.logical_and(cell >= 0, cell < pn.total_x)
    coord = (cell.astype(jnp.float32) + 0.5) / pn.total_x
    step_x = 1.0 / pn.total_x
    base, half = TIME_STEP * DIFF / KEEP, 0.5 * TIME_STEP / KEEP
    yi = lax.broadcasted_iota(jnp.int32, (ny, nz), 0)
    zi = lax.broadcasted_iota(jnp.int32, (8, nz), 1)
    y_at = (yi.astype(jnp.float32) + 0.5) / ny
    z_at = (zi.astype(jnp.float32) + 0.5) / nz

    def tables(l, carry):
        lev = levels[l]
        tab_x[l, 0] = jnp.where(inside, base - half * (lev - (coord + step_x)), 0.0)
        tab_x[l, 1] = jnp.where(inside, base + half * (lev - (coord - step_x)), 0.0)
        tab_y[l, 0] = jnp.where(yi < ny - 1, base - half * (lev - (y_at + 1.0 / ny)), 0.0)
        tab_y[l, 1] = jnp.where(yi > 0, base + half * (lev - (y_at - 1.0 / ny)), 0.0)
        tab_z[l, 0] = jnp.where(zi < nz - 1, base - half * (lev - (z_at + 1.0 / nz)), 0.0)
        tab_z[l, 1] = jnp.where(zi > 0, base + half * (lev - (z_at - 1.0 / nz)), 0.0)
        return carry

    lax.fori_loop(0, levels_ref.shape[0], tables, 0)

    for i in range(1, len(near_genes)):
        rate_copy(i - 1).wait_recv()
        rate_copy(i).start()

    def blank(i, carry):
        par, k, s = lax.div(i, slots * TOP), lax.rem(lax.div(i, TOP), slots), lax.rem(i, TOP)
        zero = jnp.zeros((halo * ny, nz), jnp.float32)

        @pl.when(jnp.logical_not(has_left))
        def _():
            near[par, k, s, left_rows] = zero

        @pl.when(jnp.logical_not(has_right))
        def _():
            near[par, k, s, right_rows] = zero

        return carry

    lax.fori_loop(0, 2 * slots * TOP, blank, 0)

    scale = KEEP**SUBSTEPS
    own_cell = lax.broadcasted_iota(jnp.int32, (width * ny, nz), 0) // ny + p * width
    own_x = (own_cell.astype(jnp.float32) + 0.5) / pn.total_x
    hill = 0.1 + own_x * own_x / (0.09 + own_x * own_x)
    for b in range(BLOCKS):
        bit = STATE_BITS - 1 - gene_order[b]
        act = on[bit] * hill
        rate = act + off[bit]
        share = act / rate
        gone = 1.0 - jnp.exp(-rate)
        up = share * gone
        down = (1.0 - share) * gone
        tab_s[b, 0, 0] = (1.0 - up) * scale
        tab_s[b, 0, 1] = down * scale
        tab_s[b, 1, 0] = (1.0 - down) * scale
        tab_s[b, 1, 1] = up * scale

    rate_copy(len(near_genes) - 1).wait_recv()
    lax.fori_loop(0, slots, lambda k, c: (look_up(1, k), c)[1], 0)
    mine = near.at[0, :, :, own]
    pltpu.make_async_copy(mine, mine, own_sem).wait()

    def spread(src, start, n, c):
        at, size = start * ny, n * ny

        def read(off):
            return src[pl.ds(at + off, size)]

        here = read(0)
        out = here + c[0][pl.ds(at, size)] * read(ny) + c[1][pl.ds(at, size)] * read(-ny)
        by_y, by_z = (n, ny, nz), (size // 8, 8, nz)
        along_y = c[2][None] * read(1).reshape(by_y) + c[3][None] * read(-1).reshape(by_y)
        z_next = pltpu.roll(here, nz - 1, axis=1).reshape(by_z)
        z_last = pltpu.roll(here, 1, axis=1).reshape(by_z)
        along_z = c[4][None] * z_next + c[5][None] * z_last
        return out + along_y.reshape(size, nz) + along_z.reshape(size, nz)

    def diffuse(b, k, batch):
        par, to = lax.rem(b, 2), jnp.minimum(b, 1)
        coef = []
        for m in range(BATCH):
            at = ((to * slots + k) * TOP + batch * BATCH + m) * 3
            lev = [lev_tab[at + d] for d in range(3)]
            coef.append(
                (
                    tab_x.at[lev[0], 0], tab_x.at[lev[0], 1], tab_y[lev[1], 0], tab_y[lev[1], 1],
                    tab_z[lev[2], 0], tab_z[lev[2], 1],
                )
            )
        for i in range(SUBSTEPS):
            extra = SUBSTEPS - 1 - i
            start, stop = halo - extra, halo + width + extra
            for at in range(start, stop, PIECE):
                n = min(PIECE, stop - at)
                for m in range(BATCH):
                    s = batch * BATCH + m
                    src = near.at[par, k, s] if i == 0 else work.at[(i + 1) % 2, m]
                    new = spread(src, at, n, coef[m])
                    if i < SUBSTEPS - 1:
                        work[i % 2, m, rows(at, n)] = new
                    else:
                        post[to, k, s, rows(at - halo, n)] = new

    def move(k, s):
        return pltpu.make_async_remote_copy(
            src_ref=post.at[0, k, s],
            dst_ref=post.at[1, k, s],
            send_sem=move_send,
            recv_sem=move_recv.at[k],
            device_id=(peers[ORDER[s] // mids], p),
            device_id_type=MESH,
        )

    def picked(b):
        order = gene_order[b]
        picks = [order == q for q in range(BLOCKS)]

        def of_mask(values):
            out = values[-1]
            for q in range(BLOCKS - 1):
                out = lax.select(picks[q], values[q], out)
            return out

        return of_mask

    def is_high(of_mask, r):
        values = []
        for mask in MASKS:
            bit = jnp.int32(1 if r & mask else 0)
            if mask >= mids:
                mine = lax.rem(lax.div(g, mask // mids), 2)
                bit = 1 - mine if r & mask else mine
            values.append(bit)
        return of_mask(values)

    def mix(b, k, states, store):
        of_mask = picked(b)
        high = {r: is_high(of_mask, r) for r in states}
        wanted = [r for r in range(TOP) if r in states or any(r ^ mask in states for mask in MASKS)]

        span = ny * (2 if width % 2 == 0 and len(states) <= 4 else 1)

        def strip(i, c):
            at = pl.multiple_of(i * span, span)
            cut = pl.ds(at, span)
            held = {r: post[1, k, ORDER.index(r), cut] for r in wanted}
            for r in states:
                mate = of_mask([held[r ^ mask] for mask in MASKS])
                store(r, at, span, tab_s[b, high[r], 0, cut] * held[r] + tab_s[b, high[r], 1, cut] * mate)
            return c

        lax.fori_loop(0, width * ny // span, strip, 0)

    def place(par, k):
        def store(r, at, span, value):
            near[par, k, ORDER.index(r), pl.ds(pl.multiple_of(halo * ny + at, ny), span)] = value

        return store

    def switch(i, carry):
        b, k = lax.div(i, slots), lax.rem(i, slots)
        par = lax.rem(b + 1, 2)

        @pl.when(b == 0)
        def _():
            dst = post.at[1, k, pl.ds(0, away)]
            pltpu.make_async_copy(dst, dst, move_recv.at[k]).wait()

        pl.when(jnp.logical_and(b > 0, k == 0))(lambda: sent_edges(par))
        mix(b, k, list(range(TOP)), place(par, k))

        @pl.when(b < BLOCKS - 2)
        def _():
            send_edges(par, k, pl.ds(0, TOP), halo_recv.at[par, k])

        @pl.when(b == BLOCKS - 2)
        def _():
            def each(batch, c):
                send_edges(par, k, pl.ds(batch * BATCH, BATCH), last_recv.at[k, batch])
                return c

            lax.fori_loop(0, batches, each, 0)

        return carry

    end_par = BLOCKS % 2

    def out_copy(k, r):
        return pltpu.make_async_remote_copy(
            src_ref=near.at[end_par, k, ORDER.index(r), own],
            dst_ref=out_ref.at[r % mids, g * slots + k],
            send_sem=out_send,
            recv_sem=out_recv,
            device_id=(peers[r // mids], p),
            device_id_type=MESH,
        )

    def finish_states(k, states):
        sent = [r for r in states if r >= mids]
        kept = [r for r in states if r < mids]
        if sent:
            mix(BLOCKS - 1, k, sent, place(end_par, k))
            for r in sent:
                out_copy(k, r).start()

        def keep(r, at, span, value):
            out_ref[r, g * slots + k, pl.ds(at, span)] = value

        if kept:
            mix(BLOCKS - 1, k, kept, keep)

    finals = final_after()
    opening = min(i for i in range(batches) if finals[i])

    def sub(b, k, batch):
        first, end, par = b == 0, b == BLOCKS - 1, lax.rem(b, 2)

        @pl.when(jnp.logical_and(jnp.logical_not(end), batch == 0))
        def _():
            both_ways(lambda at: near.at[par, k, :, at], halo_recv.at[par, k])

        @pl.when(end)
        def _():
            both_ways(lambda at: near.at[par, k, pl.ds(batch * BATCH, BATCH), at], last_recv.at[k, batch])

        diffuse(b, k, batch)
        for i in range(batches):

            @pl.when(jnp.logical_and(first, batch == i))
            def _(i=i):
                for s in range(i * BATCH, (i + 1) * BATCH):
                    if ORDER[s] >= mids:
                        move(k, s).start()
                    else:
                        post[1, k, s] = post[0, k, s]

            if finals[i]:

                @pl.when(jnp.logical_and(end, batch == i))
                def _(i=i):
                    if i == opening:
                        pl.when(k == 0)(lambda: sent_edges(end_par))
                    finish_states(k, finals[i])

    def step(i, carry):
        b, k = lax.div(i, slots), lax.rem(i, slots)
        lax.fori_loop(0, batches, lambda batch, c: (sub(b, k, batch), c)[1], 0)

        first, last, end = b == 0, k == slots - 1, b == BLOCKS - 1
        start = jnp.where(first, jnp.maximum(k - 1, 0), i)
        stop = jnp.where(first, jnp.where(last, k + 1, k), jnp.where(end, i, i + 1))
        lax.fori_loop(start, stop, switch, 0)
        return carry

    lax.fori_loop(0, BLOCKS * slots, step, 0)

    sent_edges(1 - end_par)
    src = post.at[0, :, pl.ds(0, away)]
    pltpu.make_async_copy(src, src, move_send).wait()
    src = rates.at[pl.ds(0, genes - 1)]
    pltpu.make_async_copy(src, src, rate_send).wait()
    src = near.at[end_par, :, pl.ds(0, away), own]
    pltpu.make_async_copy(src, src, out_send).wait()
    dst = out_ref.at[:, pl.ds(0, (genes - 1) * slots)]
    pltpu.make_async_copy(dst, dst, out_recv).wait()


def local(density, levels, rate_index, on_rate, off_rate, gene_order):
    count, width_x, size_y, size_z = density.shape
    pn = Plan(lax.axis_size("gene"), lax.axis_size("prot"), count, width_x, size_y, size_z)
    shape = (pn.mids, pn.units, width_x * size_y, size_z)
    inputs = (density.reshape(shape), rate_index.T, levels, on_rate, off_rate, gene_order)
    f32, i32 = jnp.float32, jnp.int32
    tall = (pn.layers * size_y, size_z)
    dma = pltpu.SemaphoreType.DMA
    out = pl.pallas_call(
        partial(body, pn),
        out_shape=pltpu.VMEM(shape, f32),
        in_specs=[pl.BlockSpec(memory_space=pltpu.HBM)] * len(inputs),
        out_specs=pl.BlockSpec(memory_space=pltpu.VMEM),
        scratch_shapes=[
            pltpu.VMEM((2, pn.slots, TOP) + tall, f32),
            pltpu.VMEM((2, pn.slots, TOP, width_x * size_y, size_z), f32),
            pltpu.VMEM((2, BATCH) + tall, f32),
            pltpu.VMEM(levels.shape + (2,) + tall, f32),
            pltpu.VMEM(levels.shape + (2, size_y, size_z), f32),
            pltpu.VMEM(levels.shape + (2, 8, size_z), f32),
            pltpu.VMEM((BLOCKS, 2, 2, width_x * size_y, size_z), f32),
            pltpu.SMEM((pn.genes, 3, count), i32),
            pltpu.SMEM(levels.shape, f32),
            pltpu.SMEM(on_rate.shape, f32),
            pltpu.SMEM(off_rate.shape, f32),
            pltpu.SMEM(gene_order.shape, i32),
            pltpu.SMEM((2 * pn.slots * TOP * 3,), i32),
            dma((len(inputs) - 1,)),
            dma(()),
            dma((2,)),
            dma((2, pn.slots)),
            dma((pn.slots, TOP // BATCH)),
            dma(()),
            dma((pn.slots,)),
            dma(()),
            dma(()),
            dma(()),
            dma((pn.genes.bit_length() - 1,)),
        ],
        compiler_params=pltpu.CompilerParams(
            collective_id=0, has_side_effects=True, vmem_limit_bytes=56 * 1024 * 1024
        ),
        name="exchange_evolve",
    )(*[pltpu.with_memory_space_constraint(a, pltpu.HBM) for a in inputs])
    return out.reshape(density.shape)


def solution(mesh):
    in_specs = (P("gene", "prot", None, None), P(), P("gene", None), P(), P(), P())
    out_specs = P("gene", "prot", None, None)
    return jax.shard_map(local, mesh=mesh, in_specs=in_specs, out_specs=out_specs, check_vma=False)
```

```python
from functools import partial

import jax
import jax.numpy as jnp
from jax import lax
from jax.experimental import pallas as pl
from jax.experimental.pallas import tpu as pltpu
from jax.sharding import PartitionSpec as P

STATE_BITS = 8
BLOCKS = 4
SUBSTEPS = 6
DIFF = 1.0
TIME_STEP = 0.15
KEEP = 1.0 - 6.0 * TIME_STEP * DIFF
TOP = 2**BLOCKS
BATCH = 2
PIECE = 1
ORDER = (12, 8, 4, 13, 14, 9, 5, 15, 10, 6, 11, 7, 0, 1, 2, 3)
MASKS = tuple(TOP >> (q + 1) for q in range(BLOCKS))
MESH = pl.DeviceIdType.MESH


def final_after():
    batch_of = {r: s // BATCH for s, r in enumerate(ORDER)}
    last = {r: max(batch_of[a] for a in [r] + [r ^ mask for mask in MASKS]) for r in range(TOP)}
    return [[r for r in ORDER if last[r] == i] for i in range(TOP // BATCH)]


class Plan:
    def __init__(self, genes, prots, count, width, size_y, size_z):
        self.genes, self.prots = genes, prots
        self.units = count * genes // TOP
        self.mids = count // self.units
        self.slots = self.units // genes
        self.width, self.size_y, self.size_z = width, size_y, size_z
        self.total_x = width * prots
        self.halo = SUBSTEPS
        self.layers = width + 2 * self.halo
        assert self.slots * genes == self.units and self.mids * genes == TOP
        assert width >= self.halo


def body(
    pn, x_ref, rate_ref, levels_ref, on_ref, off_ref, order_ref, out_ref,
    near, post, work, tab_x, tab_y, tab_z, tab_s, rates, levels, on, off, gene_order, lev_tab,
    small_sem, own_sem, halo_send, halo_recv, last_recv, move_send, move_recv, out_send, out_recv, rate_send, rate_recv,
):
    g, p = lax.axis_index("gene"), lax.axis_index("prot")
    ny, nz = pn.size_y, pn.size_z
    genes, mids, slots, halo, width = pn.genes, pn.mids, pn.slots, pn.halo, pn.width
    has_left, has_right = p > 0, p < pn.prots - 1
    has_both = jnp.logical_and(has_left, has_right)
    has_one = jnp.logical_and(jnp.logical_or(has_left, has_right), jnp.logical_not(has_both))
    near_genes = [1 << i for i in range(genes.bit_length() - 1)]
    batches, part = TOP // BATCH, TOP // 2
    fine = max((BLOCKS - 1) * slots - 2, slots)
    away = (genes - 1) * mids

    def rows(layer, n):
        return pl.ds(layer * ny, n * ny)

    def flip(a, d):
        out, bit = 0, 1
        while bit < genes:
            i, j = lax.rem(lax.div(a, bit), 2), lax.rem(lax.div(d, bit), 2)
            out = out + (i + j - 2 * i * j) * bit
            bit *= 2
        return out

    peers = [g] + [flip(g, d) for d in range(1, genes)]
    own, left_rows, right_rows = rows(halo, width), rows(0, halo), rows(halo + width, halo)

    small = [
        pltpu.make_async_copy(src, dst, small_sem.at[i])
        for i, (src, dst) in enumerate(
            [
                (rate_ref, rates.at[0]), (levels_ref, levels), (on_ref, on), (off_ref, off),
                (order_ref, gene_order),
            ]
        )
    ]
    for copy in small:
        copy.start()

    barrier = pltpu.get_barrier_semaphore()
    for d in near_genes:
        pl.semaphore_signal(barrier, inc=1, device_id=(peers[d], p), device_id_type=MESH)

    @pl.when(has_left)
    def _():
        pl.semaphore_signal(barrier, inc=1, device_id=(g, p - 1), device_id_type=MESH)

    @pl.when(has_right)
    def _():
        pl.semaphore_signal(barrier, inc=1, device_id=(g, p + 1), device_id_type=MESH)

    pl.semaphore_wait(barrier, len(near_genes) + jnp.where(has_left, 1, 0) + jnp.where(has_right, 1, 0))

    def edge(src, par, way, k, where, recv_sem):
        return pltpu.make_async_remote_copy(
            src_ref=src,
            dst_ref=near.at[par, k, where, right_rows if way else left_rows],
            send_sem=halo_send.at[par],
            recv_sem=recv_sem,
            device_id=(g, p - 1 if way else p + 1),
            device_id_type=MESH,
        )

    first_layer = (width - halo, 0)
    can_send = (has_right, has_left)

    def send_edges(par, k, where, recv_sem):
        for way in range(2):
            src = near.at[par, k, where, rows(halo + first_layer[way], halo)]
            pl.when(can_send[way])(edge(src, par, way, k, where, recv_sem).start)

    def both_ways(ref_of, sem):
        one, two = ref_of(rows(0, halo)), ref_of(rows(0, 2 * halo))
        pl.when(has_one)(pltpu.make_async_copy(one, one, sem).wait)
        pl.when(has_both)(pltpu.make_async_copy(two, two, sem).wait)

    def sent_edges(par):
        both_ways(lambda at: near.at[par, :, :, at], halo_send.at[par])

    def own_copy(k, s):
        unit = peers[ORDER[s] // mids] * slots + k
        return pltpu.make_async_copy(
            x_ref.at[ORDER[s] % mids, unit], near.at[0, k, s, own], own_sem
        )

    def open_slot(k, carry):
        for way in range(2):

            @pl.when(can_send[way])
            def _(way=way):
                for s, r in enumerate(ORDER):
                    unit = peers[r // mids] * slots + k
                    src = x_ref.at[r % mids, unit, rows(first_layer[way], halo)]
                    edge(src, 0, way, k, s, halo_recv.at[0, k, s // part]).start()

        for s in range(TOP):
            own_copy(k, s).start()
        return carry

    lax.fori_loop(0, slots, open_slot, 0)
    for copy in small:
        copy.wait()

    def rate_copy(i):
        return pltpu.make_async_remote_copy(
            src_ref=rates.at[pl.ds(0, near_genes[i])],
            dst_ref=rates.at[pl.ds(near_genes[i], near_genes[i])],
            send_sem=rate_send,
            recv_sem=rate_recv.at[i],
            device_id=(peers[near_genes[i]], p),
            device_id_type=MESH,
        )

    def look_up(late, k):
        for s, r in enumerate(ORDER):
            row = r // mids if late else 0
            unit = (g if late else peers[r // mids]) * slots + k
            for d in range(3):
                lev_tab[((late * slots + k) * TOP + s) * 3 + d] = rates[row, d, r % mids * pn.units + unit]

    rate_copy(0).start()
    lax.fori_loop(0, slots, lambda k, c: (look_up(0, k), c)[1], 0)

    cell = lax.broadcasted_iota(jnp.int32, (pn.layers * ny, nz), 0) // ny - halo + p * width
    inside = jnp.logical_and(cell >= 0, cell < pn.total_x)
    coord = (cell.astype(jnp.float32) + 0.5) / pn.total_x
    step_x = 1.0 / pn.total_x
    base, half = TIME_STEP * DIFF / KEEP, 0.5 * TIME_STEP / KEEP
    yi = lax.broadcasted_iota(jnp.int32, (ny, nz), 0)
    zi = lax.broadcasted_iota(jnp.int32, (8, nz), 1)
    y_at = (yi.astype(jnp.float32) + 0.5) / ny
    z_at = (zi.astype(jnp.float32) + 0.5) / nz

    def tables(l, carry):
        lev = levels[l]
        tab_x[l, 0] = jnp.where(inside, base - half * (lev - (coord + step_x)), 0.0)
        tab_x[l, 1] = jnp.where(inside, base + half * (lev - (coord - step_x)), 0.0)
        tab_y[l, 0] = jnp.where(yi < ny - 1, base - half * (lev - (y_at + 1.0 / ny)), 0.0)
        tab_y[l, 1] = jnp.where(yi > 0, base + half * (lev - (y_at - 1.0 / ny)), 0.0)
        tab_z[l, 0] = jnp.where(zi < nz - 1, base - half * (lev - (z_at + 1.0 / nz)), 0.0)
        tab_z[l, 1] = jnp.where(zi > 0, base + half * (lev - (z_at - 1.0 / nz)), 0.0)
        return carry

    lax.fori_loop(0, levels_ref.shape[0], tables, 0)

    for i in range(1, len(near_genes)):
        rate_copy(i - 1).wait_recv()
        rate_copy(i).start()

    def blank(i, carry):
        par, k, s = lax.div(i, slots * TOP), lax.rem(lax.div(i, TOP), slots), lax.rem(i, TOP)
        zero = jnp.zeros((halo * ny, nz), jnp.float32)

        @pl.when(jnp.logical_not(has_left))
        def _():
            near[par, k, s, left_rows] = zero

        @pl.when(jnp.logical_not(has_right))
        def _():
            near[par, k, s, right_rows] = zero

        return carry

    lax.fori_loop(0, 2 * slots * TOP, blank, 0)

    scale = KEEP**SUBSTEPS
    own_cell = lax.broadcasted_iota(jnp.int32, (width * ny, nz), 0) // ny + p * width
    own_x = (own_cell.astype(jnp.float32) + 0.5) / pn.total_x
    hill = 0.1 + own_x * own_x / (0.09 + own_x * own_x)
    for b in range(BLOCKS):
        bit = STATE_BITS - 1 - gene_order[b]
        act = on[bit] * hill
        rate = act + off[bit]
        share = act / rate
        gone = 1.0 - jnp.exp(-rate)
        up = share * gone
        down = (1.0 - share) * gone
        tab_s[b, 0, 0] = (1.0 - up) * scale
        tab_s[b, 0, 1] = down * scale
        tab_s[b, 1, 0] = (1.0 - down) * scale
        tab_s[b, 1, 1] = up * scale

    rate_copy(len(near_genes) - 1).wait_recv()
    lax.fori_loop(0, slots, lambda k, c: (look_up(1, k), c)[1], 0)
    mine = near.at[0, :, :, own]
    pltpu.make_async_copy(mine, mine, own_sem).wait()

    def spread(src, start, n, c):
        at, size = start * ny, n * ny

        def read(off):
            return src[pl.ds(at + off, size)]

        here = read(0)
        out = here + c[0][pl.ds(at, size)] * read(ny) + c[1][pl.ds(at, size)] * read(-ny)
        by_y, by_z = (n, ny, nz), (size // 8, 8, nz)
        along_y = c[2][None] * read(1).reshape(by_y) + c[3][None] * read(-1).reshape(by_y)
        z_next = pltpu.roll(here, nz - 1, axis=1).reshape(by_z)
        z_last = pltpu.roll(here, 1, axis=1).reshape(by_z)
        along_z = c[4][None] * z_next + c[5][None] * z_last
        return out + along_y.reshape(size, nz) + along_z.reshape(size, nz)

    def diffuse(b, k, batch):
        par, to = lax.rem(b, 2), jnp.minimum(b, 1)
        coef = []
        for m in range(BATCH):
            at = ((to * slots + k) * TOP + batch * BATCH + m) * 3
            lev = [lev_tab[at + d] for d in range(3)]
            coef.append(
                (
                    tab_x.at[lev[0], 0], tab_x.at[lev[0], 1], tab_y[lev[1], 0], tab_y[lev[1], 1],
                    tab_z[lev[2], 0], tab_z[lev[2], 1],
                )
            )
        for i in range(SUBSTEPS):
            extra = SUBSTEPS - 1 - i
            start, stop = halo - extra, halo + width + extra
            for at in range(start, stop, PIECE):
                n = min(PIECE, stop - at)
                for m in range(BATCH):
                    s = batch * BATCH + m
                    src = near.at[par, k, s] if i == 0 else work.at[(i + 1) % 2, m]
                    new = spread(src, at, n, coef[m])
                    if i < SUBSTEPS - 1:
                        work[i % 2, m, rows(at, n)] = new
                    else:
                        post[to, k, s, rows(at - halo, n)] = new

    def move(k, s):
        return pltpu.make_async_remote_copy(
            src_ref=post.at[0, k, s],
            dst_ref=post.at[1, k, s],
            send_sem=move_send,
            recv_sem=move_recv.at[k],
            device_id=(peers[ORDER[s] // mids], p),
            device_id_type=MESH,
        )

    def picked(b):
        order = gene_order[b]
        picks = [order == q for q in range(BLOCKS)]

        def of_mask(values):
            out = values[-1]
            for q in range(BLOCKS - 1):
                out = lax.select(picks[q], values[q], out)
            return out

        return of_mask

    def is_high(of_mask, r):
        values = []
        for mask in MASKS:
            bit = jnp.int32(1 if r & mask else 0)
            if mask >= mids:
                mine = lax.rem(lax.div(g, mask // mids), 2)
                bit = 1 - mine if r & mask else mine
            values.append(bit)
        return of_mask(values)

    def mix(b, k, states, store):
        of_mask = picked(b)
        high = {r: is_high(of_mask, r) for r in states}
        wanted = [r for r in range(TOP) if r in states or any(r ^ mask in states for mask in MASKS)]

        span = ny * (2 if width % 2 == 0 and len(states) <= 4 else 1)

        def strip(i, c):
            at = pl.multiple_of(i * span, span)
            cut = pl.ds(at, span)
            held = {r: post[1, k, ORDER.index(r), cut] for r in wanted}
            for r in states:
                mate = of_mask([held[r ^ mask] for mask in MASKS])
                store(r, at, span, tab_s[b, high[r], 0, cut] * held[r] + tab_s[b, high[r], 1, cut] * mate)
            return c

        lax.fori_loop(0, width * ny // span, strip, 0)

    def place(par, k):
        def store(r, at, span, value):
            near[par, k, ORDER.index(r), pl.ds(pl.multiple_of(halo * ny + at, ny), span)] = value

        return store

    def switch(i, carry):
        b, k = lax.div(i, slots), lax.rem(i, slots)
        par = lax.rem(b + 1, 2)

        @pl.when(b == 0)
        def _():
            dst = post.at[1, k, pl.ds(0, away)]
            pltpu.make_async_copy(dst, dst, move_recv.at[k]).wait()

        pl.when(jnp.logical_and(b > 0, k == 0))(lambda: sent_edges(par))
        mix(b, k, list(range(TOP)), place(par, k))

        @pl.when(i + slots < fine)
        def _():
            for h in range(2):
                send_edges(par, k, pl.ds(h * part, part), halo_recv.at[par, k, h])

        @pl.when(jnp.logical_and(i + slots >= fine, b < BLOCKS - 1))
        def _():
            def each(batch, c):
                send_edges(par, k, pl.ds(batch * BATCH, BATCH), last_recv.at[i + slots - fine, batch])
                return c

            lax.fori_loop(0, batches, each, 0)

        return carry

    end_par = BLOCKS % 2

    def out_copy(k, r):
        return pltpu.make_async_remote_copy(
            src_ref=near.at[end_par, k, ORDER.index(r), own],
            dst_ref=out_ref.at[r % mids, g * slots + k],
            send_sem=out_send,
            recv_sem=out_recv,
            device_id=(peers[r // mids], p),
            device_id_type=MESH,
        )

    def finish_states(k, states):
        sent = [r for r in states if r >= mids]
        kept = [r for r in states if r < mids]
        if sent:
            mix(BLOCKS - 1, k, sent, place(end_par, k))
            for r in sent:
                out_copy(k, r).start()

        def keep(r, at, span, value):
            out_ref[r, g * slots + k, pl.ds(at, span)] = value

        if kept:
            mix(BLOCKS - 1, k, kept, keep)

    finals = final_after()
    opening = min(i for i in range(batches) if finals[i])

    def sub(b, k, batch):
        first, end, par = b == 0, b == BLOCKS - 1, lax.rem(b, 2)

        item = b * slots + k
        h = lax.div(batch * BATCH, part)

        @pl.when(jnp.logical_and(item < fine, lax.rem(batch * BATCH, part) == 0))
        def _():
            both_ways(lambda at: near.at[par, k, pl.ds(h * part, part), at], halo_recv.at[par, k, h])

        @pl.when(item >= fine)
        def _():
            both_ways(lambda at: near.at[par, k, pl.ds(batch * BATCH, BATCH), at], last_recv.at[item - fine, batch])

        diffuse(b, k, batch)
        for i in range(batches):

            @pl.when(jnp.logical_and(first, batch == i))
            def _(i=i):
                for s in range(i * BATCH, (i + 1) * BATCH):
                    if ORDER[s] >= mids:
                        move(k, s).start()
                    else:
                        post[1, k, s] = post[0, k, s]

            if finals[i]:

                @pl.when(jnp.logical_and(end, batch == i))
                def _(i=i):
                    if i == opening:
                        pl.when(k == 0)(lambda: sent_edges(end_par))
                    finish_states(k, finals[i])

    def step(i, carry):
        b, k = lax.div(i, slots), lax.rem(i, slots)
        lax.fori_loop(0, batches, lambda batch, c: (sub(b, k, batch), c)[1], 0)

        first, last, end = b == 0, k == slots - 1, b == BLOCKS - 1
        start = jnp.where(first, jnp.maximum(k - 1, 0), i)
        stop = jnp.where(first, jnp.where(last, k + 1, k), jnp.where(end, i, i + 1))
        lax.fori_loop(start, stop, switch, 0)
        return carry

    lax.fori_loop(0, BLOCKS * slots, step, 0)

    sent_edges(1 - end_par)
    src = post.at[0, :, pl.ds(0, away)]
    pltpu.make_async_copy(src, src, move_send).wait()
    src = rates.at[pl.ds(0, genes - 1)]
    pltpu.make_async_copy(src, src, rate_send).wait()
    src = near.at[end_par, :, pl.ds(0, away), own]
    pltpu.make_async_copy(src, src, out_send).wait()
    dst = out_ref.at[:, pl.ds(0, (genes - 1) * slots)]
    pltpu.make_async_copy(dst, dst, out_recv).wait()


def local(density, levels, rate_index, on_rate, off_rate, gene_order):
    count, width_x, size_y, size_z = density.shape
    pn = Plan(lax.axis_size("gene"), lax.axis_size("prot"), count, width_x, size_y, size_z)
    shape = (pn.mids, pn.units, width_x * size_y, size_z)
    inputs = (density.reshape(shape), rate_index.T, levels, on_rate, off_rate, gene_order)
    f32, i32 = jnp.float32, jnp.int32
    tall = (pn.layers * size_y, size_z)
    dma = pltpu.SemaphoreType.DMA
    out = pl.pallas_call(
        partial(body, pn),
        out_shape=pltpu.VMEM(shape, f32),
        in_specs=[pl.BlockSpec(memory_space=pltpu.HBM)] * len(inputs),
        out_specs=pl.BlockSpec(memory_space=pltpu.VMEM),
        scratch_shapes=[
            pltpu.VMEM((2, pn.slots, TOP) + tall, f32),
            pltpu.VMEM((2, pn.slots, TOP, width_x * size_y, size_z), f32),
            pltpu.VMEM((2, BATCH) + tall, f32),
            pltpu.VMEM(levels.shape + (2,) + tall, f32),
            pltpu.VMEM(levels.shape + (2, size_y, size_z), f32),
            pltpu.VMEM(levels.shape + (2, 8, size_z), f32),
            pltpu.VMEM((BLOCKS, 2, 2, width_x * size_y, size_z), f32),
            pltpu.SMEM((pn.genes, 3, count), i32),
            pltpu.SMEM(levels.shape, f32),
            pltpu.SMEM(on_rate.shape, f32),
            pltpu.SMEM(off_rate.shape, f32),
            pltpu.SMEM(gene_order.shape, i32),
            pltpu.SMEM((2 * pn.slots * TOP * 3,), i32),
            dma((len(inputs) - 1,)),
            dma(()),
            dma((2,)),
            dma((2, pn.slots, 2)),
            dma((pn.slots + 2, TOP // BATCH)),
            dma(()),
            dma((pn.slots,)),
            dma(()),
            dma(()),
            dma(()),
            dma((pn.genes.bit_length() - 1,)),
        ],
        compiler_params=pltpu.CompilerParams(
            collective_id=0, has_side_effects=True, vmem_limit_bytes=56 * 1024 * 1024
        ),
        name="exchange_evolve",
    )(*[pltpu.with_memory_space_constraint(a, pltpu.HBM) for a in inputs])
    return out.reshape(density.shape)


def solution(mesh):
    in_specs = (P("gene", "prot", None, None), P(), P("gene", None), P(), P(), P())
    out_specs = P("gene", "prot", None, None)
    return jax.shard_map(local, mesh=mesh, in_specs=in_specs, out_specs=out_specs, check_vma=False)
```

```python
from functools import partial

import jax
import jax.numpy as jnp
from jax import lax
from jax.experimental import pallas as pl
from jax.experimental.pallas import tpu as pltpu
from jax.sharding import PartitionSpec as P

STATE_BITS = 8
BLOCKS = 4
SUBSTEPS = 6
DIFF = 1.0
TIME_STEP = 0.15
KEEP = 1.0 - 6.0 * TIME_STEP * DIFF
TOP = 2**BLOCKS
BATCH = 2
PIECE = 1
QUAD = 4
ORDER = (12, 8, 4, 13, 14, 9, 5, 15, 10, 6, 11, 7, 0, 1, 2, 3)
MASKS = tuple(TOP >> (q + 1) for q in range(BLOCKS))
MESH = pl.DeviceIdType.MESH


def final_after():
    batch_of = {r: s // QUAD for s, r in enumerate(ORDER)}
    last = {r: max(batch_of[a] for a in [r] + [r ^ mask for mask in MASKS]) for r in range(TOP)}
    return [[r for r in ORDER if last[r] == i] for i in range(TOP // QUAD)]


class Plan:
    def __init__(self, genes, prots, count, width, size_y, size_z):
        self.genes, self.prots = genes, prots
        self.units = count * genes // TOP
        self.mids = count // self.units
        self.slots = self.units // genes
        self.width, self.size_y, self.size_z = width, size_y, size_z
        self.total_x = width * prots
        self.halo = SUBSTEPS
        self.layers = width + 2 * self.halo
        assert self.slots * genes == self.units and self.mids * genes == TOP
        assert width == self.halo and self.halo % 2 == 0


def body(
    pn, x_ref, rate_ref, levels_ref, on_ref, off_ref, order_ref, out_ref,
    near, post, work, tab_x, tab_y, tab_z, tab_s, rates, levels, on, off, gene_order, lev_tab,
    small_sem, own_sem, halo_send, halo_recv, last_recv, move_send, move_recv, out_send, out_recv, rate_send, rate_recv,
):
    g, p = lax.axis_index("gene"), lax.axis_index("prot")
    ny, nz = pn.size_y, pn.size_z
    genes, mids, slots, halo, width = pn.genes, pn.mids, pn.slots, pn.halo, pn.width
    has_left, has_right = p > 0, p < pn.prots - 1
    has_both = jnp.logical_and(has_left, has_right)
    has_one = jnp.logical_and(jnp.logical_or(has_left, has_right), jnp.logical_not(has_both))
    near_genes = [1 << i for i in range(genes.bit_length() - 1)]
    batches, quads, part = TOP // BATCH, TOP // QUAD, TOP // 2
    near_half = halo // 2
    even = lax.rem(p, 2) == 0
    fine = max((BLOCKS - 1) * slots - 2, slots)
    away = (genes - 1) * mids

    def rows(layer, n):
        return pl.ds(layer * ny, n * ny)

    def flip(a, d):
        out, bit = 0, 1
        while bit < genes:
            i, j = lax.rem(lax.div(a, bit), 2), lax.rem(lax.div(d, bit), 2)
            out = out + (i + j - 2 * i * j) * bit
            bit *= 2
        return out

    peers = [g] + [flip(g, d) for d in range(1, genes)]
    own, left_rows, right_rows = rows(halo, width), rows(0, halo), rows(halo + width, halo)

    small = [
        pltpu.make_async_copy(src, dst, small_sem.at[i])
        for i, (src, dst) in enumerate(
            [
                (rate_ref, rates.at[0]), (levels_ref, levels), (on_ref, on), (off_ref, off),
                (order_ref, gene_order),
            ]
        )
    ]
    for copy in small:
        copy.start()

    barrier = pltpu.get_barrier_semaphore()
    for d in near_genes:
        pl.semaphore_signal(barrier, inc=1, device_id=(peers[d], p), device_id_type=MESH)

    @pl.when(has_left)
    def _():
        pl.semaphore_signal(barrier, inc=1, device_id=(g, p - 1), device_id_type=MESH)

    @pl.when(has_right)
    def _():
        pl.semaphore_signal(barrier, inc=1, device_id=(g, p + 1), device_id_type=MESH)

    pl.semaphore_wait(barrier, len(near_genes) + jnp.where(has_left, 1, 0) + jnp.where(has_right, 1, 0))

    def edge(src, par, way, k, where, recv_sem):
        return pltpu.make_async_remote_copy(
            src_ref=src,
            dst_ref=near.at[par, k, where, right_rows if way else left_rows],
            send_sem=halo_send.at[par],
            recv_sem=recv_sem,
            device_id=(g, p - 1 if way else p + 1),
            device_id_type=MESH,
        )

    first_layer = (width - halo, 0)
    can_send = (has_right, has_left)

    def send_edges(par, k, where, recv_sem):
        for way in range(2):
            src = near.at[par, k, where, rows(halo + first_layer[way], halo)]
            pl.when(can_send[way])(edge(src, par, way, k, where, recv_sem).start)

    def slow(way):
        return even if way else jnp.logical_not(even)

    def send_turn(par, k, turn, quad, recv_sem):
        where = pl.ds(quad * QUAD, QUAD)
        for way in range(2):
            skip = near_half * (turn if way else 1 - turn)
            to = halo + width if way else 0
            half_copy = pltpu.make_async_remote_copy(
                src_ref=near.at[par, k, where, rows(halo + skip, near_half)],
                dst_ref=near.at[par, k, where, rows(to + skip, near_half)],
                send_sem=halo_send.at[par],
                recv_sem=recv_sem,
                device_id=(g, p - 1 if way else p + 1),
                device_id_type=MESH,
            )
            src = near.at[par, k, where, own]
            whole = edge(src, par, way, k, where, recv_sem)
            there = jnp.logical_and(can_send[way], slow(way))
            pl.when(there)(half_copy.start)
            there = jnp.logical_and(can_send[way], jnp.logical_not(slow(way)))
            pl.when(jnp.logical_and(there, turn == 0))(whole.start)

    has_slow = jnp.logical_or(jnp.logical_and(even, has_left), jnp.logical_and(jnp.logical_not(even), has_right))
    has_fast = jnp.logical_or(jnp.logical_and(even, has_right), jnp.logical_and(jnp.logical_not(even), has_left))

    def take_turn(par, k, turn, quad, sem):
        def await_layers(n):
            ref = near.at[par, k, pl.ds(quad * QUAD, QUAD), rows(0, n)]
            return pltpu.make_async_copy(ref, ref, sem).wait

        opening_turn = turn == 0
        pl.when(jnp.logical_and(opening_turn, jnp.logical_and(has_slow, has_fast)))(await_layers(halo + near_half))
        pl.when(jnp.logical_and(opening_turn, jnp.logical_and(jnp.logical_not(has_slow), has_fast)))(await_layers(halo))
        pl.when(jnp.logical_and(opening_turn, jnp.logical_and(has_slow, jnp.logical_not(has_fast))))(await_layers(near_half))
        pl.when(jnp.logical_and(turn == 1, has_slow))(await_layers(near_half))

    def both_ways(ref_of, sem):
        one, two = ref_of(rows(0, halo)), ref_of(rows(0, 2 * halo))
        pl.when(has_one)(pltpu.make_async_copy(one, one, sem).wait)
        pl.when(has_both)(pltpu.make_async_copy(two, two, sem).wait)

    def sent_edges(par):
        both_ways(lambda at: near.at[par, :, :, at], halo_send.at[par])

    def own_copy(k, s):
        unit = peers[ORDER[s] // mids] * slots + k
        return pltpu.make_async_copy(
            x_ref.at[ORDER[s] % mids, unit], near.at[0, k, s, own], own_sem
        )

    def open_slot(k, carry):
        for way in range(2):

            @pl.when(can_send[way])
            def _(way=way):
                for s, r in enumerate(ORDER):
                    unit = peers[r // mids] * slots + k
                    src = x_ref.at[r % mids, unit, rows(first_layer[way], halo)]
                    edge(src, 0, way, k, s, halo_recv.at[0, k, s // part]).start()

        for s in range(TOP):
            own_copy(k, s).start()
        return carry

    lax.fori_loop(0, slots, open_slot, 0)
    for copy in small:
        copy.wait()

    def rate_copy(i):
        return pltpu.make_async_remote_copy(
            src_ref=rates.at[pl.ds(0, near_genes[i])],
            dst_ref=rates.at[pl.ds(near_genes[i], near_genes[i])],
            send_sem=rate_send,
            recv_sem=rate_recv.at[i],
            device_id=(peers[near_genes[i]], p),
            device_id_type=MESH,
        )

    def look_up(late, k):
        for s, r in enumerate(ORDER):
            row = r // mids if late else 0
            unit = (g if late else peers[r // mids]) * slots + k
            for d in range(3):
                lev_tab[((late * slots + k) * TOP + s) * 3 + d] = rates[row, d, r % mids * pn.units + unit]

    rate_copy(0).start()
    lax.fori_loop(0, slots, lambda k, c: (look_up(0, k), c)[1], 0)

    cell = lax.broadcasted_iota(jnp.int32, (pn.layers * ny, nz), 0) // ny - halo + p * width
    inside = jnp.logical_and(cell >= 0, cell < pn.total_x)
    coord = (cell.astype(jnp.float32) + 0.5) / pn.total_x
    step_x = 1.0 / pn.total_x
    base, half = TIME_STEP * DIFF / KEEP, 0.5 * TIME_STEP / KEEP
    yi = lax.broadcasted_iota(jnp.int32, (ny, nz), 0)
    zi = lax.broadcasted_iota(jnp.int32, (8, nz), 1)
    y_at = (yi.astype(jnp.float32) + 0.5) / ny
    z_at = (zi.astype(jnp.float32) + 0.5) / nz

    def tables(l, carry):
        lev = levels[l]
        tab_x[l, 0] = jnp.where(inside, base - half * (lev - (coord + step_x)), 0.0)
        tab_x[l, 1] = jnp.where(inside, base + half * (lev - (coord - step_x)), 0.0)
        tab_y[l, 0] = jnp.where(yi < ny - 1, base - half * (lev - (y_at + 1.0 / ny)), 0.0)
        tab_y[l, 1] = jnp.where(yi > 0, base + half * (lev - (y_at - 1.0 / ny)), 0.0)
        tab_z[l, 0] = jnp.where(zi < nz - 1, base - half * (lev - (z_at + 1.0 / nz)), 0.0)
        tab_z[l, 1] = jnp.where(zi > 0, base + half * (lev - (z_at - 1.0 / nz)), 0.0)
        return carry

    lax.fori_loop(0, levels_ref.shape[0], tables, 0)

    for i in range(1, len(near_genes)):
        rate_copy(i - 1).wait_recv()
        rate_copy(i).start()

    def blank(i, carry):
        par, k, s = lax.div(i, slots * TOP), lax.rem(lax.div(i, TOP), slots), lax.rem(i, TOP)
        zero = jnp.zeros((halo * ny, nz), jnp.float32)

        @pl.when(jnp.logical_not(has_left))
        def _():
            near[par, k, s, left_rows] = zero

        @pl.when(jnp.logical_not(has_right))
        def _():
            near[par, k, s, right_rows] = zero

        return carry

    lax.fori_loop(0, 2 * slots * TOP, blank, 0)

    scale = KEEP**SUBSTEPS
    own_cell = lax.broadcasted_iota(jnp.int32, (width * ny, nz), 0) // ny + p * width
    own_x = (own_cell.astype(jnp.float32) + 0.5) / pn.total_x
    hill = 0.1 + own_x * own_x / (0.09 + own_x * own_x)
    for b in range(BLOCKS):
        bit = STATE_BITS - 1 - gene_order[b]
        act = on[bit] * hill
        rate = act + off[bit]
        share = act / rate
        gone = 1.0 - jnp.exp(-rate)
        up = share * gone
        down = (1.0 - share) * gone
        tab_s[b, 0, 0] = (1.0 - up) * scale
        tab_s[b, 0, 1] = down * scale
        tab_s[b, 1, 0] = (1.0 - down) * scale
        tab_s[b, 1, 1] = up * scale

    rate_copy(len(near_genes) - 1).wait_recv()
    lax.fori_loop(0, slots, lambda k, c: (look_up(1, k), c)[1], 0)
    mine = near.at[0, :, :, own]
    pltpu.make_async_copy(mine, mine, own_sem).wait()

    def spread(src, start, n, c):
        at, size = start * ny, n * ny
        fixed = isinstance(start, int)

        def cut(off):
            to = at + off
            return pl.ds(to if fixed or off % ny else pl.multiple_of(to, ny), size)

        def read(off):
            return src[cut(off)]

        here = read(0)
        out = here + c[0][cut(0)] * read(ny) + c[1][cut(0)] * read(-ny)
        by_y, by_z = (n, ny, nz), (size // 8, 8, nz)
        along_y = c[2][None] * read(1).reshape(by_y) + c[3][None] * read(-1).reshape(by_y)
        z_next = pltpu.roll(here, nz - 1, axis=1).reshape(by_z)
        z_last = pltpu.roll(here, 1, axis=1).reshape(by_z)
        along_z = c[4][None] * z_next + c[5][None] * z_last
        return out + along_y.reshape(size, nz) + along_z.reshape(size, nz)

    def diffuse(par, to, k, first, count, skip, cells):
        coef = []
        for m in range(count):
            at = ((to * slots + k) * TOP + first + m) * 3
            lev = [lev_tab[at + d] for d in range(3)]
            coef.append(
                (
                    tab_x.at[lev[0], 0], tab_x.at[lev[0], 1], tab_y[lev[1], 0], tab_y[lev[1], 1],
                    tab_z[lev[2], 0], tab_z[lev[2], 1],
                )
            )

        def lay(layer, n):
            return rows(layer, n) if isinstance(layer, int) else pl.ds(pl.multiple_of(layer * ny, ny), n * ny)

        for i in range(SUBSTEPS):
            extra = SUBSTEPS - 1 - i
            for at in range(-extra, cells + extra, PIECE):
                n = min(PIECE, cells + extra - at)
                for m in range(count):
                    src = near.at[par, k, first + m] if i == 0 else work.at[(i + 1) % 2, m]
                    new = spread(src, halo + skip + at, n, coef[m])
                    if i < SUBSTEPS - 1:
                        work[i % 2, m, lay(halo + skip + at, n)] = new
                    else:
                        post[to, k, first + m, lay(skip + at, n)] = new

    def move(k, s):
        return pltpu.make_async_remote_copy(
            src_ref=post.at[0, k, s],
            dst_ref=post.at[1, k, s],
            send_sem=move_send,
            recv_sem=move_recv.at[k],
            device_id=(peers[ORDER[s] // mids], p),
            device_id_type=MESH,
        )

    def picked(b):
        order = gene_order[b]
        picks = [order == q for q in range(BLOCKS)]

        def of_mask(values):
            out = values[-1]
            for q in range(BLOCKS - 1):
                out = lax.select(picks[q], values[q], out)
            return out

        return of_mask

    def is_high(of_mask, r):
        values = []
        for mask in MASKS:
            bit = jnp.int32(1 if r & mask else 0)
            if mask >= mids:
                mine = lax.rem(lax.div(g, mask // mids), 2)
                bit = 1 - mine if r & mask else mine
            values.append(bit)
        return of_mask(values)

    def mix(b, k, states, store, skip=0, cells=width):
        of_mask = picked(b)
        high = {r: is_high(of_mask, r) for r in states}
        wanted = [r for r in range(TOP) if r in states or any(r ^ mask in states for mask in MASKS)]

        span = ny

        def strip(i, c):
            at = pl.multiple_of((skip + i) * span, span)
            cut = pl.ds(at, span)
            held = {r: post[1, k, ORDER.index(r), cut] for r in wanted}
            for r in states:
                mate = of_mask([held[r ^ mask] for mask in MASKS])
                store(r, at, span, tab_s[b, high[r], 0, cut] * held[r] + tab_s[b, high[r], 1, cut] * mate)
            return c

        lax.fori_loop(0, cells, strip, 0)

    def place(par, k):
        def store(r, at, span, value):
            near[par, k, ORDER.index(r), pl.ds(pl.multiple_of(halo * ny + at, ny), span)] = value

        return store

    def switch(i, carry):
        b, k = lax.div(i, slots), lax.rem(i, slots)
        par = lax.rem(b + 1, 2)

        @pl.when(b == 0)
        def _():
            dst = post.at[1, k, pl.ds(0, away)]
            pltpu.make_async_copy(dst, dst, move_recv.at[k]).wait()

        pl.when(jnp.logical_and(b > 0, k == 0))(lambda: sent_edges(par))
        mix(b, k, list(range(TOP)), place(par, k))

        @pl.when(i + slots < fine)
        def _():
            for h in range(2):
                send_edges(par, k, pl.ds(h * part, part), halo_recv.at[par, k, h])

        @pl.when(jnp.logical_and(i + slots >= fine, b < BLOCKS - 2))
        def _():
            def each(batch, c):
                send_edges(par, k, pl.ds(batch * BATCH, BATCH), last_recv.at[i + slots - fine, batch])
                return c

            lax.fori_loop(0, batches, each, 0)

        @pl.when(b == BLOCKS - 2)
        def _():
            def turn(t, c):
                send_turn(par, k, lax.div(t, quads), lax.rem(t, quads), last_recv.at[i + slots - fine, t])
                return c

            lax.fori_loop(0, 2 * quads, turn, 0)

        return carry

    end_par = BLOCKS % 2

    def out_copy(k, r, skip):
        at = pl.multiple_of(skip * ny, ny)
        return pltpu.make_async_remote_copy(
            src_ref=near.at[end_par, k, ORDER.index(r), pl.ds(halo * ny + at, near_half * ny)],
            dst_ref=out_ref.at[r % mids, g * slots + k, pl.ds(at, near_half * ny)],
            send_sem=out_send,
            recv_sem=out_recv,
            device_id=(peers[r // mids], p),
            device_id_type=MESH,
        )

    def finish_states(k, states, skip):
        sent = [r for r in states if r >= mids]
        kept = [r for r in states if r < mids]
        if sent:
            mix(BLOCKS - 1, k, sent, place(end_par, k), skip, near_half)
            for r in sent:
                out_copy(k, r, skip).start()

        def keep(r, at, span, value):
            out_ref[r, g * slots + k, pl.ds(at, span)] = value

        if kept:
            mix(BLOCKS - 1, k, kept, keep, skip, near_half)

    finals = final_after()
    opening = min(i for i in range(quads) if finals[i])

    def sub(b, k, batch):
        first, par = b == 0, lax.rem(b, 2)
        item = b * slots + k
        h = lax.div(batch * BATCH, part)

        @pl.when(jnp.logical_and(item < fine, lax.rem(batch * BATCH, part) == 0))
        def _():
            both_ways(lambda at: near.at[par, k, pl.ds(h * part, part), at], halo_recv.at[par, k, h])

        @pl.when(item >= fine)
        def _():
            both_ways(lambda at: near.at[par, k, pl.ds(batch * BATCH, BATCH), at], last_recv.at[item - fine, batch])

        diffuse(par, jnp.minimum(b, 1), k, batch * BATCH, BATCH, 0, width)
        for i in range(batches):

            @pl.when(jnp.logical_and(first, batch == i))
            def _(i=i):
                for s in range(i * BATCH, (i + 1) * BATCH):
                    if ORDER[s] >= mids:
                        move(k, s).start()
                    else:
                        post[1, k, s] = post[0, k, s]

    def last_sub(k, t):
        turn, quad, par = lax.div(t, quads), lax.rem(t, quads), 1 - end_par
        skip = near_half * jnp.where(even, 1 - turn, turn)
        take_turn(par, k, turn, quad, last_recv.at[(BLOCKS - 1) * slots - fine + k, t])
        diffuse(par, 1, k, quad * QUAD, QUAD, skip, near_half)
        for i in range(quads):
            if finals[i]:

                @pl.when(quad == i)
                def _(i=i):
                    if i == opening:
                        pl.when(jnp.logical_and(k == 0, turn == 0))(lambda: sent_edges(end_par))
                    finish_states(k, finals[i], skip)

    def step(i, carry):
        b, k = lax.div(i, slots), lax.rem(i, slots)
        lax.fori_loop(0, batches, lambda batch, c: (sub(b, k, batch), c)[1], 0)

        first, last = b == 0, k == slots - 1
        start = jnp.where(first, jnp.maximum(k - 1, 0), i)
        stop = jnp.where(first, jnp.where(last, k + 1, k), i + 1)
        lax.fori_loop(start, stop, switch, 0)
        return carry

    lax.fori_loop(0, (BLOCKS - 1) * slots, step, 0)

    def last_step(i, carry):
        last_sub(lax.div(i, 2 * quads), lax.rem(i, 2 * quads))
        return carry

    lax.fori_loop(0, slots * 2 * quads, last_step, 0)

    sent_edges(1 - end_par)
    src = post.at[0, :, pl.ds(0, away)]
    pltpu.make_async_copy(src, src, move_send).wait()
    src = rates.at[pl.ds(0, genes - 1)]
    pltpu.make_async_copy(src, src, rate_send).wait()
    src = near.at[end_par, :, pl.ds(0, away), own]
    pltpu.make_async_copy(src, src, out_send).wait()
    dst = out_ref.at[:, pl.ds(0, (genes - 1) * slots)]
    pltpu.make_async_copy(dst, dst, out_recv).wait()


def local(density, levels, rate_index, on_rate, off_rate, gene_order):
    count, width_x, size_y, size_z = density.shape
    pn = Plan(lax.axis_size("gene"), lax.axis_size("prot"), count, width_x, size_y, size_z)
    shape = (pn.mids, pn.units, width_x * size_y, size_z)
    inputs = (density.reshape(shape), rate_index.T, levels, on_rate, off_rate, gene_order)
    f32, i32 = jnp.float32, jnp.int32
    tall = (pn.layers * size_y, size_z)
    dma = pltpu.SemaphoreType.DMA
    out = pl.pallas_call(
        partial(body, pn),
        out_shape=pltpu.VMEM(shape, f32),
        in_specs=[pl.BlockSpec(memory_space=pltpu.HBM)] * len(inputs),
        out_specs=pl.BlockSpec(memory_space=pltpu.VMEM),
        scratch_shapes=[
            pltpu.VMEM((2, pn.slots, TOP) + tall, f32),
            pltpu.VMEM((2, pn.slots, TOP, width_x * size_y, size_z), f32),
            pltpu.VMEM((2, QUAD) + tall, f32),
            pltpu.VMEM(levels.shape + (2,) + tall, f32),
            pltpu.VMEM(levels.shape + (2, size_y, size_z), f32),
            pltpu.VMEM(levels.shape + (2, 8, size_z), f32),
            pltpu.VMEM((BLOCKS, 2, 2, width_x * size_y, size_z), f32),
            pltpu.SMEM((pn.genes, 3, count), i32),
            pltpu.SMEM(levels.shape, f32),
            pltpu.SMEM(on_rate.shape, f32),
            pltpu.SMEM(off_rate.shape, f32),
            pltpu.SMEM(gene_order.shape, i32),
            pltpu.SMEM((2 * pn.slots * TOP * 3,), i32),
            dma((len(inputs) - 1,)),
            dma(()),
            dma((2,)),
            dma((2, pn.slots, 2)),
            dma((pn.slots + 2, TOP // BATCH)),
            dma(()),
            dma((pn.slots,)),
            dma(()),
            dma(()),
            dma(()),
            dma((pn.genes.bit_length() - 1,)),
        ],
        compiler_params=pltpu.CompilerParams(
            collective_id=0, has_side_effects=True, vmem_limit_bytes=56 * 1024 * 1024
        ),
        name="exchange_evolve",
    )(*[pltpu.with_memory_space_constraint(a, pltpu.HBM) for a in inputs])
    return out.reshape(density.shape)


def solution(mesh):
    in_specs = (P("gene", "prot", None, None), P(), P("gene", None), P(), P(), P())
    out_specs = P("gene", "prot", None, None)
    return jax.shard_map(local, mesh=mesh, in_specs=in_specs, out_specs=out_specs, check_vma=False)
```

```python
from functools import partial

import jax
import jax.numpy as jnp
from jax import lax
from jax.experimental import pallas as pl
from jax.experimental.pallas import tpu as pltpu
from jax.sharding import PartitionSpec as P

STATE_BITS = 8
BLOCKS = 4
SUBSTEPS = 6
DIFF = 1.0
TIME_STEP = 0.15
KEEP = 1.0 - 6.0 * TIME_STEP * DIFF
TOP = 2**BLOCKS
BATCH = 4
PIECE = 1
QUAD = 4
ORDER = (12, 8, 4, 13, 14, 9, 5, 15, 10, 6, 11, 7, 0, 1, 2, 3)
MASKS = tuple(TOP >> (q + 1) for q in range(BLOCKS))
MESH = pl.DeviceIdType.MESH


def final_after():
    batch_of = {r: s // QUAD for s, r in enumerate(ORDER)}
    last = {r: max(batch_of[a] for a in [r] + [r ^ mask for mask in MASKS]) for r in range(TOP)}
    return [[r for r in ORDER if last[r] == i] for i in range(TOP // QUAD)]


class Plan:
    def __init__(self, genes, prots, count, width, size_y, size_z):
        self.genes, self.prots = genes, prots
        self.units = count * genes // TOP
        self.mids = count // self.units
        self.slots = self.units // genes
        self.width, self.size_y, self.size_z = width, size_y, size_z
        self.total_x = width * prots
        self.halo = SUBSTEPS
        self.layers = width + 2 * self.halo
        assert self.slots * genes == self.units and self.mids * genes == TOP
        assert width == self.halo and self.halo % 2 == 0


def body(
    pn, x_ref, rate_ref, levels_ref, on_ref, off_ref, order_ref, out_ref,
    near, post, work, tab_x, tab_y, tab_z, tab_s, rates, levels, on, off, gene_order, lev_tab,
    small_sem, own_sem, halo_send, halo_recv, last_recv, move_send, move_recv, out_send, out_recv, rate_send, rate_recv,
):
    g, p = lax.axis_index("gene"), lax.axis_index("prot")
    ny, nz = pn.size_y, pn.size_z
    genes, mids, slots, halo, width = pn.genes, pn.mids, pn.slots, pn.halo, pn.width
    has_left, has_right = p > 0, p < pn.prots - 1
    has_both = jnp.logical_and(has_left, has_right)
    has_one = jnp.logical_and(jnp.logical_or(has_left, has_right), jnp.logical_not(has_both))
    near_genes = [1 << i for i in range(genes.bit_length() - 1)]
    batches, quads, part = TOP // BATCH, TOP // QUAD, TOP // 2
    near_half = halo // 2
    even = lax.rem(p, 2) == 0
    fine = max((BLOCKS - 1) * slots - 2, slots)
    away = (genes - 1) * mids

    def rows(layer, n):
        return pl.ds(layer * ny, n * ny)

    def flip(a, d):
        out, bit = 0, 1
        while bit < genes:
            i, j = lax.rem(lax.div(a, bit), 2), lax.rem(lax.div(d, bit), 2)
            out = out + (i + j - 2 * i * j) * bit
            bit *= 2
        return out

    peers = [g] + [flip(g, d) for d in range(1, genes)]
    own, left_rows, right_rows = rows(halo, width), rows(0, halo), rows(halo + width, halo)

    small = [
        pltpu.make_async_copy(src, dst, small_sem.at[i])
        for i, (src, dst) in enumerate(
            [
                (rate_ref, rates.at[0]), (levels_ref, levels), (on_ref, on), (off_ref, off),
                (order_ref, gene_order),
            ]
        )
    ]
    for copy in small:
        copy.start()

    barrier = pltpu.get_barrier_semaphore()
    for d in near_genes:
        pl.semaphore_signal(barrier, inc=1, device_id=(peers[d], p), device_id_type=MESH)

    @pl.when(has_left)
    def _():
        pl.semaphore_signal(barrier, inc=1, device_id=(g, p - 1), device_id_type=MESH)

    @pl.when(has_right)
    def _():
        pl.semaphore_signal(barrier, inc=1, device_id=(g, p + 1), device_id_type=MESH)

    pl.semaphore_wait(barrier, len(near_genes) + jnp.where(has_left, 1, 0) + jnp.where(has_right, 1, 0))

    def edge(src, par, way, k, where, recv_sem):
        return pltpu.make_async_remote_copy(
            src_ref=src,
            dst_ref=near.at[par, k, where, right_rows if way else left_rows],
            send_sem=halo_send.at[par],
            recv_sem=recv_sem,
            device_id=(g, p - 1 if way else p + 1),
            device_id_type=MESH,
        )

    first_layer = (width - halo, 0)
    can_send = (has_right, has_left)

    def send_edges(par, k, where, recv_sem):
        for way in range(2):
            src = near.at[par, k, where, rows(halo + first_layer[way], halo)]
            pl.when(can_send[way])(edge(src, par, way, k, where, recv_sem).start)

    def slow(way):
        return even if way else jnp.logical_not(even)

    def send_turn(par, k, turn, quad, recv_sem):
        where = pl.ds(quad * QUAD, QUAD)
        for way in range(2):
            skip = near_half * (turn if way else 1 - turn)
            to = halo + width if way else 0
            half_copy = pltpu.make_async_remote_copy(
                src_ref=near.at[par, k, where, rows(halo + skip, near_half)],
                dst_ref=near.at[par, k, where, rows(to + skip, near_half)],
                send_sem=halo_send.at[par],
                recv_sem=recv_sem,
                device_id=(g, p - 1 if way else p + 1),
                device_id_type=MESH,
            )
            src = near.at[par, k, where, own]
            whole = edge(src, par, way, k, where, recv_sem)
            there = jnp.logical_and(can_send[way], slow(way))
            pl.when(there)(half_copy.start)
            there = jnp.logical_and(can_send[way], jnp.logical_not(slow(way)))
            pl.when(jnp.logical_and(there, turn == 0))(whole.start)

    has_slow = jnp.logical_or(jnp.logical_and(even, has_left), jnp.logical_and(jnp.logical_not(even), has_right))
    has_fast = jnp.logical_or(jnp.logical_and(even, has_right), jnp.logical_and(jnp.logical_not(even), has_left))

    def take_turn(par, k, turn, quad, sem):
        def await_layers(n):
            ref = near.at[par, k, pl.ds(quad * QUAD, QUAD), rows(0, n)]
            return pltpu.make_async_copy(ref, ref, sem).wait

        opening_turn = turn == 0
        pl.when(jnp.logical_and(opening_turn, jnp.logical_and(has_slow, has_fast)))(await_layers(halo + near_half))
        pl.when(jnp.logical_and(opening_turn, jnp.logical_and(jnp.logical_not(has_slow), has_fast)))(await_layers(halo))
        pl.when(jnp.logical_and(opening_turn, jnp.logical_and(has_slow, jnp.logical_not(has_fast))))(await_layers(near_half))
        pl.when(jnp.logical_and(turn == 1, has_slow))(await_layers(near_half))

    def both_ways(ref_of, sem):
        one, two = ref_of(rows(0, halo)), ref_of(rows(0, 2 * halo))
        pl.when(has_one)(pltpu.make_async_copy(one, one, sem).wait)
        pl.when(has_both)(pltpu.make_async_copy(two, two, sem).wait)

    def sent_edges(par):
        both_ways(lambda at: near.at[par, :, :, at], halo_send.at[par])

    def own_copy(k, s):
        unit = peers[ORDER[s] // mids] * slots + k
        return pltpu.make_async_copy(
            x_ref.at[ORDER[s] % mids, unit], near.at[0, k, s, own], own_sem
        )

    def open_slot(k, carry):
        for way in range(2):

            @pl.when(can_send[way])
            def _(way=way):
                for s, r in enumerate(ORDER):
                    unit = peers[r // mids] * slots + k
                    src = x_ref.at[r % mids, unit, rows(first_layer[way], halo)]
                    edge(src, 0, way, k, s, halo_recv.at[0, k, s // part]).start()

        for s in range(TOP):
            own_copy(k, s).start()
        return carry

    lax.fori_loop(0, slots, open_slot, 0)
    for copy in small:
        copy.wait()

    def rate_copy(i):
        return pltpu.make_async_remote_copy(
            src_ref=rates.at[pl.ds(0, near_genes[i])],
            dst_ref=rates.at[pl.ds(near_genes[i], near_genes[i])],
            send_sem=rate_send,
            recv_sem=rate_recv.at[i],
            device_id=(peers[near_genes[i]], p),
            device_id_type=MESH,
        )

    def look_up(late, k):
        for s, r in enumerate(ORDER):
            row = r // mids if late else 0
            unit = (g if late else peers[r // mids]) * slots + k
            for d in range(3):
                lev_tab[((late * slots + k) * TOP + s) * 3 + d] = rates[row, d, r % mids * pn.units + unit]

    rate_copy(0).start()
    lax.fori_loop(0, slots, lambda k, c: (look_up(0, k), c)[1], 0)

    cell = lax.broadcasted_iota(jnp.int32, (pn.layers * ny, nz), 0) // ny - halo + p * width
    inside = jnp.logical_and(cell >= 0, cell < pn.total_x)
    coord = (cell.astype(jnp.float32) + 0.5) / pn.total_x
    step_x = 1.0 / pn.total_x
    base, half = TIME_STEP * DIFF / KEEP, 0.5 * TIME_STEP / KEEP
    yi = lax.broadcasted_iota(jnp.int32, (ny, nz), 0)
    zi = lax.broadcasted_iota(jnp.int32, (8, nz), 1)
    y_at = (yi.astype(jnp.float32) + 0.5) / ny
    z_at = (zi.astype(jnp.float32) + 0.5) / nz

    def tables(l, carry):
        lev = levels[l]
        tab_x[l, 0] = jnp.where(inside, base - half * (lev - (coord + step_x)), 0.0)
        tab_x[l, 1] = jnp.where(inside, base + half * (lev - (coord - step_x)), 0.0)
        tab_y[l, 0] = jnp.where(yi < ny - 1, base - half * (lev - (y_at + 1.0 / ny)), 0.0)
        tab_y[l, 1] = jnp.where(yi > 0, base + half * (lev - (y_at - 1.0 / ny)), 0.0)
        tab_z[l, 0] = jnp.where(zi < nz - 1, base - half * (lev - (z_at + 1.0 / nz)), 0.0)
        tab_z[l, 1] = jnp.where(zi > 0, base + half * (lev - (z_at - 1.0 / nz)), 0.0)
        return carry

    lax.fori_loop(0, levels_ref.shape[0], tables, 0)

    for i in range(1, len(near_genes)):
        rate_copy(i - 1).wait_recv()
        rate_copy(i).start()

    def blank(i, carry):
        par, k, s = lax.div(i, slots * TOP), lax.rem(lax.div(i, TOP), slots), lax.rem(i, TOP)
        zero = jnp.zeros((halo * ny, nz), jnp.float32)

        @pl.when(jnp.logical_not(has_left))
        def _():
            near[par, k, s, left_rows] = zero

        @pl.when(jnp.logical_not(has_right))
        def _():
            near[par, k, s, right_rows] = zero

        return carry

    lax.fori_loop(0, 2 * slots * TOP, blank, 0)

    scale = KEEP**SUBSTEPS
    own_cell = lax.broadcasted_iota(jnp.int32, (width * ny, nz), 0) // ny + p * width
    own_x = (own_cell.astype(jnp.float32) + 0.5) / pn.total_x
    hill = 0.1 + own_x * own_x / (0.09 + own_x * own_x)
    for b in range(BLOCKS):
        bit = STATE_BITS - 1 - gene_order[b]
        act = on[bit] * hill
        rate = act + off[bit]
        share = act / rate
        gone = 1.0 - jnp.exp(-rate)
        up = share * gone
        down = (1.0 - share) * gone
        tab_s[b, 0, 0] = (1.0 - up) * scale
        tab_s[b, 0, 1] = down * scale
        tab_s[b, 1, 0] = (1.0 - down) * scale
        tab_s[b, 1, 1] = up * scale

    rate_copy(len(near_genes) - 1).wait_recv()
    lax.fori_loop(0, slots, lambda k, c: (look_up(1, k), c)[1], 0)
    mine = near.at[0, :, :, own]
    pltpu.make_async_copy(mine, mine, own_sem).wait()

    def spread(src, start, n, c):
        at, size = start * ny, n * ny
        fixed = isinstance(start, int)

        def cut(off):
            to = at + off
            return pl.ds(to if fixed or off % ny else pl.multiple_of(to, ny), size)

        def read(off):
            return src[cut(off)]

        here = read(0)
        out = here + c[0][cut(0)] * read(ny) + c[1][cut(0)] * read(-ny)
        by_y, by_z = (n, ny, nz), (size // 8, 8, nz)
        along_y = c[2][None] * read(1).reshape(by_y) + c[3][None] * read(-1).reshape(by_y)
        z_next = pltpu.roll(here, nz - 1, axis=1).reshape(by_z)
        z_last = pltpu.roll(here, 1, axis=1).reshape(by_z)
        along_z = c[4][None] * z_next + c[5][None] * z_last
        return out + along_y.reshape(size, nz) + along_z.reshape(size, nz)

    def diffuse(par, to, k, first, count, skip, cells):
        coef = []
        for m in range(count):
            at = ((to * slots + k) * TOP + first + m) * 3
            lev = [lev_tab[at + d] for d in range(3)]
            coef.append(
                (
                    tab_x.at[lev[0], 0], tab_x.at[lev[0], 1], tab_y[lev[1], 0], tab_y[lev[1], 1],
                    tab_z[lev[2], 0], tab_z[lev[2], 1],
                )
            )

        def lay(layer, n):
            return rows(layer, n) if isinstance(layer, int) else pl.ds(pl.multiple_of(layer * ny, ny), n * ny)

        for i in range(SUBSTEPS):
            extra = SUBSTEPS - 1 - i
            for at in range(-extra, cells + extra, PIECE):
                n = min(PIECE, cells + extra - at)
                for m in range(count):
                    src = near.at[par, k, first + m] if i == 0 else work.at[(i + 1) % 2, m]
                    new = spread(src, halo + skip + at, n, coef[m])
                    if i < SUBSTEPS - 1:
                        work[i % 2, m, lay(halo + skip + at, n)] = new
                    else:
                        post[to, k, first + m, lay(skip + at, n)] = new

    def move(k, s):
        return pltpu.make_async_remote_copy(
            src_ref=post.at[0, k, s],
            dst_ref=post.at[1, k, s],
            send_sem=move_send,
            recv_sem=move_recv.at[k],
            device_id=(peers[ORDER[s] // mids], p),
            device_id_type=MESH,
        )

    def picked(b):
        order = gene_order[b]
        picks = [order == q for q in range(BLOCKS)]

        def of_mask(values):
            out = values[-1]
            for q in range(BLOCKS - 1):
                out = lax.select(picks[q], values[q], out)
            return out

        return of_mask

    def is_high(of_mask, r):
        values = []
        for mask in MASKS:
            bit = jnp.int32(1 if r & mask else 0)
            if mask >= mids:
                mine = lax.rem(lax.div(g, mask // mids), 2)
                bit = 1 - mine if r & mask else mine
            values.append(bit)
        return of_mask(values)

    def mix(b, k, states, store, skip=0, cells=width):
        of_mask = picked(b)
        high = {r: is_high(of_mask, r) for r in states}
        wanted = [r for r in range(TOP) if r in states or any(r ^ mask in states for mask in MASKS)]

        span = ny

        def strip(i, c):
            at = pl.multiple_of((skip + i) * span, span)
            cut = pl.ds(at, span)
            held = {r: post[1, k, ORDER.index(r), cut] for r in wanted}
            for r in states:
                mate = of_mask([held[r ^ mask] for mask in MASKS])
                store(r, at, span, tab_s[b, high[r], 0, cut] * held[r] + tab_s[b, high[r], 1, cut] * mate)
            return c

        lax.fori_loop(0, cells, strip, 0)

    def place(par, k):
        def store(r, at, span, value):
            near[par, k, ORDER.index(r), pl.ds(pl.multiple_of(halo * ny + at, ny), span)] = value

        return store

    def switch(i, carry):
        b, k = lax.div(i, slots), lax.rem(i, slots)
        par = lax.rem(b + 1, 2)

        @pl.when(b == 0)
        def _():
            dst = post.at[1, k, pl.ds(0, away)]
            pltpu.make_async_copy(dst, dst, move_recv.at[k]).wait()

        pl.when(jnp.logical_and(b > 0, k == 0))(lambda: sent_edges(par))
        mix(b, k, list(range(TOP)), place(par, k))

        @pl.when(i + slots < fine)
        def _():
            for h in range(2):
                send_edges(par, k, pl.ds(h * part, part), halo_recv.at[par, k, h])

        @pl.when(jnp.logical_and(i + slots >= fine, b < BLOCKS - 2))
        def _():
            def each(batch, c):
                send_edges(par, k, pl.ds(batch * BATCH, BATCH), last_recv.at[i + slots - fine, batch])
                return c

            lax.fori_loop(0, batches, each, 0)

        @pl.when(b == BLOCKS - 2)
        def _():
            def turn(t, c):
                send_turn(par, k, lax.div(t, quads), lax.rem(t, quads), last_recv.at[i + slots - fine, t])
                return c

            lax.fori_loop(0, 2 * quads, turn, 0)

        return carry

    end_par = BLOCKS % 2

    def out_copy(k, r, skip):
        at = pl.multiple_of(skip * ny, ny)
        return pltpu.make_async_remote_copy(
            src_ref=near.at[end_par, k, ORDER.index(r), pl.ds(halo * ny + at, near_half * ny)],
            dst_ref=out_ref.at[r % mids, g * slots + k, pl.ds(at, near_half * ny)],
            send_sem=out_send,
            recv_sem=out_recv,
            device_id=(peers[r // mids], p),
            device_id_type=MESH,
        )

    def finish_states(k, states, skip):
        sent = [r for r in states if r >= mids]
        kept = [r for r in states if r < mids]
        if sent:
            mix(BLOCKS - 1, k, sent, place(end_par, k), skip, near_half)
            for r in sent:
                out_copy(k, r, skip).start()

        def keep(r, at, span, value):
            out_ref[r, g * slots + k, pl.ds(at, span)] = value

        if kept:
            mix(BLOCKS - 1, k, kept, keep, skip, near_half)

    finals = final_after()
    opening = min(i for i in range(quads) if finals[i])

    def sub(b, k, batch):
        first, par = b == 0, lax.rem(b, 2)
        item = b * slots + k
        h = lax.div(batch * BATCH, part)

        @pl.when(jnp.logical_and(item < fine, lax.rem(batch * BATCH, part) == 0))
        def _():
            both_ways(lambda at: near.at[par, k, pl.ds(h * part, part), at], halo_recv.at[par, k, h])

        @pl.when(item >= fine)
        def _():
            both_ways(lambda at: near.at[par, k, pl.ds(batch * BATCH, BATCH), at], last_recv.at[item - fine, batch])

        diffuse(par, jnp.minimum(b, 1), k, batch * BATCH, BATCH, 0, width)
        for i in range(batches):

            @pl.when(jnp.logical_and(first, batch == i))
            def _(i=i):
                for s in range(i * BATCH, (i + 1) * BATCH):
                    if ORDER[s] >= mids:
                        move(k, s).start()
                    else:
                        post[1, k, s] = post[0, k, s]

    def last_sub(k, t):
        turn, quad, par = lax.div(t, quads), lax.rem(t, quads), 1 - end_par
        skip = near_half * jnp.where(even, 1 - turn, turn)
        take_turn(par, k, turn, quad, last_recv.at[(BLOCKS - 1) * slots - fine + k, t])
        diffuse(par, 1, k, quad * QUAD, QUAD, skip, near_half)
        for i in range(quads):
            if finals[i]:

                @pl.when(quad == i)
                def _(i=i):
                    if i == opening:
                        pl.when(jnp.logical_and(k == 0, turn == 0))(lambda: sent_edges(end_par))
                    finish_states(k, finals[i], skip)

    def step(i, carry):
        b, k = lax.div(i, slots), lax.rem(i, slots)
        lax.fori_loop(0, batches, lambda batch, c: (sub(b, k, batch), c)[1], 0)

        first, last = b == 0, k == slots - 1
        start = jnp.where(first, jnp.maximum(k - 1, 0), i)
        stop = jnp.where(first, jnp.where(last, k + 1, k), i + 1)
        lax.fori_loop(start, stop, switch, 0)
        return carry

    lax.fori_loop(0, (BLOCKS - 1) * slots, step, 0)

    def last_step(i, carry):
        last_sub(lax.div(i, 2 * quads), lax.rem(i, 2 * quads))
        return carry

    lax.fori_loop(0, slots * 2 * quads, last_step, 0)

    sent_edges(1 - end_par)
    src = post.at[0, :, pl.ds(0, away)]
    pltpu.make_async_copy(src, src, move_send).wait()
    src = rates.at[pl.ds(0, genes - 1)]
    pltpu.make_async_copy(src, src, rate_send).wait()
    src = near.at[end_par, :, pl.ds(0, away), own]
    pltpu.make_async_copy(src, src, out_send).wait()
    dst = out_ref.at[:, pl.ds(0, (genes - 1) * slots)]
    pltpu.make_async_copy(dst, dst, out_recv).wait()


def local(density, levels, rate_index, on_rate, off_rate, gene_order):
    count, width_x, size_y, size_z = density.shape
    pn = Plan(lax.axis_size("gene"), lax.axis_size("prot"), count, width_x, size_y, size_z)
    shape = (pn.mids, pn.units, width_x * size_y, size_z)
    inputs = (density.reshape(shape), rate_index.T, levels, on_rate, off_rate, gene_order)
    f32, i32 = jnp.float32, jnp.int32
    tall = (pn.layers * size_y, size_z)
    dma = pltpu.SemaphoreType.DMA
    out = pl.pallas_call(
        partial(body, pn),
        out_shape=pltpu.VMEM(shape, f32),
        in_specs=[pl.BlockSpec(memory_space=pltpu.HBM)] * len(inputs),
        out_specs=pl.BlockSpec(memory_space=pltpu.VMEM),
        scratch_shapes=[
            pltpu.VMEM((2, pn.slots, TOP) + tall, f32),
            pltpu.VMEM((2, pn.slots, TOP, width_x * size_y, size_z), f32),
            pltpu.VMEM((2, QUAD) + tall, f32),
            pltpu.VMEM(levels.shape + (2,) + tall, f32),
            pltpu.VMEM(levels.shape + (2, size_y, size_z), f32),
            pltpu.VMEM(levels.shape + (2, 8, size_z), f32),
            pltpu.VMEM((BLOCKS, 2, 2, width_x * size_y, size_z), f32),
            pltpu.SMEM((pn.genes, 3, count), i32),
            pltpu.SMEM(levels.shape, f32),
            pltpu.SMEM(on_rate.shape, f32),
            pltpu.SMEM(off_rate.shape, f32),
            pltpu.SMEM(gene_order.shape, i32),
            pltpu.SMEM((2 * pn.slots * TOP * 3,), i32),
            dma((len(inputs) - 1,)),
            dma(()),
            dma((2,)),
            dma((2, pn.slots, 2)),
            dma((pn.slots + 2, 2 * TOP // QUAD)),
            dma(()),
            dma((pn.slots,)),
            dma(()),
            dma(()),
            dma(()),
            dma((pn.genes.bit_length() - 1,)),
        ],
        compiler_params=pltpu.CompilerParams(
            collective_id=0, has_side_effects=True, vmem_limit_bytes=56 * 1024 * 1024
        ),
        name="exchange_evolve",
    )(*[pltpu.with_memory_space_constraint(a, pltpu.HBM) for a in inputs])
    return out.reshape(density.shape)


def solution(mesh):
    in_specs = (P("gene", "prot", None, None), P(), P("gene", None), P(), P(), P())
    out_specs = P("gene", "prot", None, None)
    return jax.shard_map(local, mesh=mesh, in_specs=in_specs, out_specs=out_specs, check_vma=False)
```
